32 devices in a mesh: curve: 4 (over y, core), group: 8 (over z, x).
Axes of the slice: x: 2, y: 2, z: 4, core: 2. Of those that a mesh axis runs over, the one named last changes fastest.
Arguments:
- right_side: float32 [125, 16384], P(None, ('curve', 'group')), may hold values from -6 to 6, as said below
- conductivity: float32 [16384], P(('curve', 'group')), may hold values from 0.3 to 3
- destination: int32 [16384], P(('curve', 'group')), may hold values from 0 to 16383, as said below
- neighbour: int32 [6, 16384], P(None, ('curve', 'group')), may hold values from -1 to 1023, as said below
- orientation: int32 [6, 16384], P(None, ('curve', 'group')), may hold values from 0 to 3, as said below
- send_list: int32 [2, 8192], P(None, ('curve', 'group')), may hold values from 0 to 511, as said below
Outputs:
- solution: float32 [125, 16384], P(None, ('curve', 'group'))
- residual: float32 [125, 16384], P(None, ('curve', 'group'))
The draws below stay inside these ranges and needn't reach their ends.
Inputs may be any that keep to these rules, and one draw needn't show every extreme that they name: `right_side`: custom normal-like values. `destination`: A permutation of all cells. Devices are ordered along the curve with curve slowest; every cell's new device is its old device or the one just before or after it. From each device at most 64 cells go to the next device and exactly as many come back from it; 64 is reached at some pair of neighbouring devices in every draw. `neighbour`: values below 512 are local cells of the same device. Only face 0 may name a slot from 512 to 512 + 256 - 1 (filled by the previous device from its send_list row 1), only face 1 a slot from 768 up (filled by the next device from its send_list row 0). Faces are paired: the cell across face f sees this cell across face f xor 1. -1 only at the domain boundary; the first device has no partner across its face 0 slots and the last none across face 1 slots. `orientation`: both sides of a shared face carry the same code; ignored where neighbour is -1. `send_list`: per device 256 distinct local cells in each row.
All inputs are finite; a program needn't handle non-finite values.
Results may differ from the reference program's by a relative error of at most 0.00015.
Values sent between devices are 32-bit elements; how exact they have to be, the bound alone decides.
No kernel may reach another device: no remote copies, remote signals or barrier semaphores. Data moves between devices by JAX's collectives and lax.ppermute only.
A program may use at most 64 MiB of HBM per device.

```python
import math
import jax
import jax.numpy as jnp
from jax import lax

CELLS_DEV = 512
SIDE = 16
NODES = 5
ITERS = 2
BLOCK = 125
GHOST = 256
MOVE = 64
RANKS = 32
CELLS = 16384


def draw_right_side(key, part):
    key_rough = jax.random.fold_in(jax.random.fold_in(key, 3), 0)
    rough = jax.random.normal(key_rough, (BLOCK, CELLS), jnp.float32)
    return jnp.clip(rough, -6.0, 6.0)


def draw_destination(key, part):
    base_key = jax.random.fold_in(key, 29)
    key_swap, key_pick, key_rank, key_order = jax.random.split(base_key, 4)
    swap_counts = jax.random.randint(key_swap, (RANKS - 1,), 0, MOVE + 1).astype(jnp.int32)
    forced_at = jax.random.randint(key_pick, (), 0, RANKS - 1)
    swap_counts = swap_counts.at[forced_at].set(MOVE)
    zero_pad = jnp.zeros((1,), jnp.int32)
    to_left = jnp.concatenate([zero_pad, swap_counts])[:, None]
    to_right = jnp.concatenate([swap_counts, zero_pad])[:, None]
    local_rank = jax.vmap(lambda one_key: jax.random.permutation(one_key, CELLS_DEV))(jax.random.split(key_rank, RANKS)).astype(jnp.int32)
    old_owner = jnp.arange(RANKS, dtype=jnp.int32)[:, None]
    target = jnp.where(local_rank < to_left, old_owner - 1, jnp.where(local_rank >= CELLS_DEV - to_right, old_owner + 1, old_owner)).reshape(CELLS)
    shuffled = jax.random.permutation(key_order, CELLS).astype(jnp.int32)
    new_order = shuffled[jnp.argsort(target[shuffled], stable=True)]
    return jnp.zeros((CELLS,), jnp.int32).at[new_order].set(jnp.arange(CELLS, dtype=jnp.int32))


def mesh_arrays(key):
    base_key = jax.random.fold_in(key, 17)
    key_perm, key_code = jax.random.split(base_key)
    ghost_count = SIDE * SIDE
    layers = CELLS_DEV // ghost_count
    site_cell = jax.vmap(lambda one_key: jax.random.permutation(one_key, CELLS_DEV))(jax.random.split(key_perm, RANKS)).astype(jnp.int32)
    face_codes = jax.random.randint(key_code, (RANKS, CELLS_DEV, 3), 0, 4).astype(jnp.int32)
    site_ids = jnp.arange(CELLS_DEV, dtype=jnp.int32)
    layer_pos = (site_ids // ghost_count)[None, :]
    row_pos = (site_ids // SIDE % SIDE)[None, :]
    col_pos = (site_ids % SIDE)[None, :]
    plane_slot = row_pos * SIDE + col_pos
    rank_ids = jnp.arange(RANKS, dtype=jnp.int32)[:, None]

    def ahead_by(table, step):
        return jnp.roll(table, -step, axis=1)

    def behind_by(table, step):
        return jnp.roll(table, step, axis=1)
    face_zero = jnp.where(layer_pos > 0, behind_by(site_cell, ghost_count), jnp.where(rank_ids > 0, CELLS_DEV + plane_slot, -1))
    face_one = jnp.where(layer_pos < layers - 1, ahead_by(site_cell, ghost_count), jnp.where(rank_ids < RANKS - 1, CELLS_DEV + ghost_count + plane_slot, -1))
    face_two = jnp.where(row_pos > 0, behind_by(site_cell, SIDE), -1)
    face_three = jnp.where(row_pos < SIDE - 1, ahead_by(site_cell, SIDE), -1)
    face_four = jnp.where(col_pos > 0, behind_by(site_cell, 1), -1)
    face_five = jnp.where(col_pos < SIDE - 1, ahead_by(site_cell, 1), -1)
    code_x = face_codes[..., 0]
    code_y = face_codes[..., 1]
    code_z = face_codes[..., 2]
    previous_x = jnp.roll(jnp.roll(code_x, 1, axis=0), -(layers - 1) * ghost_count, axis=1)
    code_zero = jnp.where(layer_pos > 0, behind_by(code_x, ghost_count), previous_x)
    code_two = jnp.where(row_pos > 0, behind_by(code_y, SIDE), code_y)
    code_four = jnp.where(col_pos > 0, behind_by(code_z, 1), code_z)
    inverse = jnp.argsort(site_cell, axis=1, stable=True)
    neighbour_sites = jnp.stack([face_zero, face_one, face_two, face_three, face_four, face_five]).astype(jnp.int32)
    code_sites = jnp.stack([code_zero, code_x, code_two, code_y, code_four, code_z]).astype(jnp.int32)
    neighbour = jnp.take_along_axis(neighbour_sites, inverse[None], axis=2).reshape(6, CELLS)
    orientation = jnp.take_along_axis(code_sites, inverse[None], axis=2).reshape(6, CELLS)
    send_list = jnp.stack([site_cell[:, :ghost_count], site_cell[:, (layers - 1) * ghost_count:]]).reshape(2, RANKS * ghost_count)
    return (neighbour, orientation, send_list)


def draw_neighbour(key, part):
    return mesh_arrays(key)[0]


def draw_orientation(key, part):
    return mesh_arrays(key)[1]


def draw_send_list(key, part):
    return mesh_arrays(key)[2]


def levels(stream_key, dims, cuts, smallest, high):
    def one(dim, shards_of):
        heights = jax.random.uniform(jax.random.fold_in(jax.random.fold_in(stream_key, 6), dim), (shards_of,), jnp.float32, smallest / len(cuts), high / len(cuts))
        return jnp.repeat(jnp.exp(heights), dims[dim] // shards_of).reshape((-1,) + (1,) * (len(dims) - dim - 1))

    gain = one(*cuts[0])
    for cut in cuts[1:]:
        gain = gain * one(*cut)
    return gain


def setup_inputs(seed: int = 0) -> dict:
    arg_keys = jax.random.split(jax.random.key(seed), 7)
    right_side = draw_right_side(jax.random.fold_in(arg_keys[6], 71), 0)
    conductivity = jnp.clip(jnp.exp(math.log(3.0) - 2.3025851 * jax.random.uniform(arg_keys[1], (CELLS,), jnp.float32) ** levels(arg_keys[1], (CELLS,), ((0, 32),), -0.2, 0.2)), 0.3, 3.0)
    destination = draw_destination(jax.random.fold_in(arg_keys[6], 71), 0)
    neighbour = draw_neighbour(jax.random.fold_in(arg_keys[6], 71), 0)
    orientation = draw_orientation(jax.random.fold_in(arg_keys[6], 71), 0)
    send_list = draw_send_list(jax.random.fold_in(arg_keys[6], 71), 0)
    return {"right_side": right_side, "conductivity": conductivity, "destination": destination, "neighbour": neighbour, "orientation": orientation, "send_list": send_list}


PENALTY = 80.0
HIGHEST = lax.Precision.HIGHEST
GAUSS_POINTS = (-0.9061798459386640, -0.5384693101056831, 0.0, 0.5384693101056831, 0.9061798459386640)
GAUSS_WEIGHTS = (0.2369268850561891, 0.4786286704993665, 0.5688888888888889, 0.4786286704993665, 0.2369268850561891)


def lagrange_value(points, position, location):
    product_value = 1.0
    for other_id in range(len(points)):
        if other_id != position:
            product_value = product_value * (location - points[other_id]) / (points[position] - points[other_id])
    return product_value


def lagrange_slope(points, position, location):
    slope_sum = 0.0
    for skipped in range(len(points)):
        if skipped == position:
            continue
        addend = 1.0 / (points[position] - points[skipped])
        for other_id in range(len(points)):
            if other_id != position and other_id != skipped:
                addend = addend * (location - points[other_id]) / (points[position] - points[other_id])
        slope_sum = slope_sum + addend
    return slope_sum


def basis_tables():
    points = [0.5 * (value + 1.0) for value in GAUSS_POINTS]
    weights = [0.5 * value for value in GAUSS_WEIGHTS]
    count = len(points)
    slopes = [[lagrange_slope(points, column, points[row_id]) for column in range(count)] for row_id in range(count)]
    start_value = [lagrange_value(points, column, 0.0) for column in range(count)]
    end_value = [lagrange_value(points, column, 1.0) for column in range(count)]
    start_slope = [-lagrange_slope(points, column, 0.0) for column in range(count)]
    end_slope = [lagrange_slope(points, column, 1.0) for column in range(count)]
    listed = (weights, slopes, start_value, end_value, start_slope, end_slope)
    return tuple(jnp.asarray(table, jnp.float32) for table in listed)


def face_vectors(face_id, tables):
    if face_id % 2:
        return tables[3], tables[5]
    return tables[2], tables[4]


def face_data(block_field, conduct, face_id, tables):
    trace_vec, normal_vec = face_vectors(face_id, tables)
    axis_id = face_id // 2
    trace_value = jnp.tensordot(trace_vec, block_field, axes=([0], [axis_id]), precision=HIGHEST)
    trace_flux = conduct * jnp.tensordot(normal_vec, block_field, axes=([0], [axis_id]), precision=HIGHEST)
    return trace_value, trace_flux


def spread_back(vector, face_part, axis_id):
    bcast_shape = [1, 1, 1, 1]
    bcast_shape[axis_id] = NODES
    return vector.reshape(bcast_shape) * jnp.expand_dims(face_part, axis_id)


def volume_term(block_field, conduct, tables):
    weights, slopes = tables[0], tables[1]
    weight_3d = (weights[:, None, None] * weights[None, :, None] * weights[None, None, :])[..., None]
    result = weight_3d * block_field
    forward = ("qp,pjkc->qjkc", "qp,ipkc->iqkc", "qp,ijpc->ijqc")
    backward = ("qp,qjkc->pjkc", "qp,iqkc->ipkc", "qp,ijqc->ijpc")
    for axis_id in range(3):
        grads = jnp.einsum(forward[axis_id], slopes, block_field, precision=HIGHEST)
        result = result + jnp.einsum(backward[axis_id], slopes, weight_3d * conduct * grads, precision=HIGHEST)
    return result


def face_term(trace_value, trace_flux, conduct, other_value, other_flux, other_conduct, partner, orient_code, face_id, tables):
    weights = tables[0]
    trace_vec, normal_vec = face_vectors(face_id, tables)
    axis_id = face_id // 2
    flip_first = (orient_code % 2) == 1
    flip_second = (orient_code // 2) == 1
    other_value = jnp.where(flip_first, other_value[::-1], other_value)
    other_value = jnp.where(flip_second, other_value[:, ::-1], other_value)
    other_flux = jnp.where(flip_first, other_flux[::-1], other_flux)
    other_flux = jnp.where(flip_second, other_flux[:, ::-1], other_flux)
    outside = partner < 0
    other_value = jnp.where(outside, -trace_value, other_value)
    other_flux = jnp.where(outside, -trace_flux, other_flux)
    other_conduct = jnp.where(outside, conduct, other_conduct)
    penalty = PENALTY * jnp.maximum(conduct, other_conduct)
    trace_jump = trace_value - other_value
    mean_flux = 0.5 * (trace_flux - other_flux)
    face_weight = (weights[:, None] * weights[None, :])[:, :, None]
    first_part = spread_back(trace_vec, face_weight * (penalty * trace_jump - mean_flux), axis_id)
    return first_part + spread_back(normal_vec, face_weight * (-0.5 * conduct * trace_jump), axis_id)


def global_partners(neighbour, send_list):
    cell_ids = jnp.arange(CELLS, dtype=jnp.int32)
    owner = cell_ids // CELLS_DEV
    lower = jnp.maximum(owner - 1, 0)
    upper = jnp.minimum(owner + 1, RANKS - 1)
    left_slot = jnp.clip(neighbour - CELLS_DEV, 0, GHOST - 1)
    right_slot = jnp.clip(neighbour - CELLS_DEV - GHOST, 0, GHOST - 1)
    from_left = lower * CELLS_DEV + send_list[1][lower * GHOST + left_slot]
    from_right = upper * CELLS_DEV + send_list[0][upper * GHOST + right_slot]
    local_ids = owner * CELLS_DEV + neighbour
    joined = jnp.where(neighbour < CELLS_DEV, local_ids, jnp.where(neighbour < CELLS_DEV + GHOST, from_left, from_right))
    return jnp.where(neighbour < 0, -1, joined).astype(jnp.int32)


def operate(block_field, conduct, partners, orientation, tables):
    faces = [face_data(block_field, conduct, face_id, tables) for face_id in range(6)]
    result = volume_term(block_field, conduct, tables)
    for face_id in range(6):
        partner = partners[face_id]
        safe_idx = jnp.where(partner < 0, 0, partner)
        other_value, other_flux = faces[face_id ^ 1]
        result = result + face_term(faces[face_id][0], faces[face_id][1], conduct,
                                    other_value[:, :, safe_idx], other_flux[:, :, safe_idx], conduct[safe_idx],
                                    partner, orientation[face_id], face_id, tables)
    return result


def reference(right_side, conductivity, destination, neighbour, orientation, send_list):
    tables = basis_tables()
    placed = jnp.zeros((BLOCK, CELLS), jnp.float32).at[:, destination].set(right_side)
    conduct = jnp.zeros((CELLS,), jnp.float32).at[destination].set(conductivity)
    partners = global_partners(neighbour, send_list)
    source = placed.reshape(NODES, NODES, NODES, CELLS)
    solution = jnp.zeros_like(source)
    residual = source
    direction = source
    norm_now = jnp.sum(residual * residual)
    for step in range(ITERS):
        image = operate(direction, conduct, partners, orientation, tables)
        step_size = norm_now / jnp.sum(direction * image)
        solution = solution + step_size * direction
        residual = residual - step_size * image
        if step + 1 < ITERS:
            norm_next = jnp.sum(residual * residual)
            direction = residual + (norm_next / norm_now) * direction
            norm_now = norm_next
    return solution.reshape(BLOCK, CELLS), residual.reshape(BLOCK, CELLS)
```

```python
import functools

import jax
import jax.numpy as jnp
import numpy as np
from jax import lax
from jax.experimental import pallas as pl
from jax.experimental.pallas import tpu as pltpu
from jax.sharding import PartitionSpec as P

NODES = 5
FACE = NODES * NODES
BLOCK = NODES**3
MOVE = 64
LANES = 128
ROWS = 128
HALF = 32
SLAB = 2 * HALF
FACES = 6
PENALTY = 80.0
AXES = ("curve", "group")
VMEM_LIMIT = 24 * 1024 * 1024

GAUSS_POINTS = (-0.906179845938664, -0.5384693101056831, 0.0, 0.5384693101056831, 0.906179845938664)
GAUSS_WEIGHTS = (
    0.2369268850561891,
    0.4786286704993665,
    0.5688888888888889,
    0.4786286704993665,
    0.2369268850561891,
)


def lagrange_value(points, position, location):
    value = 1.0
    for other in range(len(points)):
        if other != position:
            value = value * (location - points[other]) / (points[position] - points[other])
    return value


def lagrange_slope(points, position, location):
    total = 0.0
    for skipped in range(len(points)):
        if skipped == position:
            continue
        addend = 1.0 / (points[position] - points[skipped])
        for other in range(len(points)):
            if other != position and other != skipped:
                addend = addend * (location - points[other]) / (points[position] - points[other])
        total = total + addend
    return total


def basis_tables():
    points = [0.5 * (value + 1.0) for value in GAUSS_POINTS]
    weights = [0.5 * value for value in GAUSS_WEIGHTS]
    count = len(points)
    slopes = [[lagrange_slope(points, p, points[q]) for p in range(count)] for q in range(count)]
    start_value = [lagrange_value(points, p, 0.0) for p in range(count)]
    end_value = [lagrange_value(points, p, 1.0) for p in range(count)]
    start_slope = [-lagrange_slope(points, p, 0.0) for p in range(count)]
    end_slope = [lagrange_slope(points, p, 1.0) for p in range(count)]
    listed = (weights, slopes, start_value, end_value, start_slope, end_slope)
    return [np.asarray(np.asarray(table, np.float32), np.float64) for table in listed]


def along_axis(matrix, axis_id):
    factors = [np.eye(NODES)] * 3
    factors[axis_id] = matrix
    return np.kron(factors[0], np.kron(factors[1], factors[2]))


def parity_basis():
    root = np.sqrt(0.5)
    line = np.zeros((NODES, NODES))
    line[0, 0] = line[0, 4] = line[1, 1] = line[1, 3] = root
    line[2, 2] = 1.0
    line[3, 0], line[3, 4] = root, -root
    line[4, 1], line[4, 3] = root, -root
    odd = np.array([0, 0, 0, 1, 1])
    return np.kron(line, line), np.repeat(odd, NODES), np.tile(odd, NODES)


def split_two(matrix):
    high = matrix.astype(np.float32).astype(jnp.bfloat16)
    low = (matrix - high.astype(np.float64)).astype(np.float32).astype(jnp.bfloat16)
    return high, low


@functools.cache
def operator_constants():
    weights, slopes, *ends = basis_tables()
    cell_weight = np.kron(weights, np.kron(weights, weights))
    face_weight = np.kron(weights, weights)
    parity, odd_first, odd_second = parity_basis()
    stiff = np.zeros((BLOCK, BLOCK))
    for axis_id in range(3):
        grad = along_axis(slopes, axis_id)
        stiff += grad.T @ (cell_weight[:, None] * grad)
    trace = np.zeros((FACES * SLAB + ROWS, ROWS))
    back = np.zeros((ROWS, FACES * SLAB))
    for face in range(FACES):
        tangent = along_axis(ends[face % 2][None, :], face // 2)
        normal = along_axis(ends[2 + face % 2][None, :], face // 2)
        start = face * SLAB
        trace[start : start + FACE, :BLOCK] = parity @ tangent
        trace[start + HALF : start + HALF + FACE, :BLOCK] = parity @ normal
        spread = (face_weight[:, None] * parity.T)
        back[:BLOCK, start : start + FACE] = tangent.T @ spread
        back[:BLOCK, start + HALF : start + HALF + FACE] = -0.5 * normal.T @ spread
    trace[FACES * SLAB : FACES * SLAB + BLOCK, :BLOCK] = stiff
    high, low = split_two(trace)
    trace3 = np.concatenate([high, high, low], 1)
    backs = []
    for first, last in ((0, 2), (2, FACES)):
        high, low = split_two(back[:, first * SLAB : last * SLAB])
        backs.append(np.concatenate([high, high, low], 1))
    weight_rows = np.zeros((ROWS, 1), np.float32)
    weight_rows[:BLOCK, 0] = cell_weight
    flips = np.zeros((SLAB, LANES), np.float32)
    for start in (0, HALF):
        flips[start : start + FACE, 0] = odd_first
        flips[start : start + FACE, 1] = odd_second
    return trace3, backs[0], backs[1], weight_rows, flips


def as_bf16(value):
    return value.astype(jnp.bfloat16)


def as_f32(value):
    return value.astype(jnp.float32)


def parts_of(value, count):
    pieces = []
    for step in range(count):
        piece = as_bf16(value)
        pieces.append(piece)
        if step + 1 < count:
            value = value - as_f32(piece)
    return pieces


def dot(left, right):
    return lax.dot_general(left, right, (((1,), (0,)), ((), ())), preferred_element_type=jnp.float32)


def dot_rows(left, right):
    return lax.dot_general(left, right, (((1,), (1,)), ((), ())), preferred_element_type=jnp.float32)


def times3(table3, value):
    high, low = parts_of(value, 2)
    return dot(table3, jnp.concatenate([high, low, high], 0))


def pick(value, chosen, count):
    rows = value.shape[0]
    out = dot(jnp.concatenate(parts_of(value, count), 0), chosen)
    total = out[(count - 1) * rows :]
    for step in reversed(range(count - 1)):
        total = total + out[step * rows : (step + 1) * rows]
    return total


def one_hot(index_row, rows, offset=0):
    ids = lax.broadcasted_iota(jnp.int32, (rows, index_row.shape[1]), 0)
    return as_bf16(jnp.where(ids == index_row - offset, 1.0, 0.0))


def whole(ref_list):
    return [pl.BlockSpec(memory_space=pltpu.VMEM) for _ in ref_list]


def call(kernel, outs, args, flops, scratch=(), name=None):
    moved = sum(a.size * a.dtype.itemsize for a in args) + sum(o.size * o.dtype.itemsize for o in outs)
    return pl.pallas_call(
        kernel,
        out_shape=list(outs),
        in_specs=whole(args),
        out_specs=whole(outs),
        scratch_shapes=list(scratch),
        compiler_params=pltpu.CompilerParams(vmem_limit_bytes=VMEM_LIMIT),
        cost_estimate=pl.CostEstimate(flops=flops, bytes_accessed=moved, transcendentals=0),
        name=name,
    )(*args)


def f32(*shape):
    return jax.ShapeDtypeStruct(shape, jnp.float32)


def targets(dest_ref):
    cells = dest_ref.shape[1]
    rank = lax.axis_index("curve") * lax.axis_size("group") + lax.axis_index("group")
    dest = dest_ref[...]
    owner = lax.div(dest, cells)
    return owner - rank, dest - owner * cells


def fill_payload(payload, rhs_ref, cond_ref, slot):
    payload[:BLOCK] = rhs_ref[...]
    payload[BLOCK : BLOCK + 1] = cond_ref[...]
    payload[BLOCK + 1 : BLOCK + 2] = as_f32(slot + 1)
    payload[BLOCK + 2 : ROWS] = jnp.zeros((ROWS - BLOCK - 2, payload.shape[1]), jnp.float32)


def pack_kernel(rhs_ref, cond_ref, dest_ref, left_ref, right_ref, payload):
    cells = dest_ref.shape[1]
    tiles = cells // LANES
    target, slot = targets(dest_ref)
    fill_payload(payload, rhs_ref, cond_ref, slot)
    leaving = [target == -1, target == 1]
    marks = [as_f32(mask) for mask in leaving]
    stacked = jnp.concatenate(
        [mark[:, t * LANES : (t + 1) * LANES] for mark in marks for t in range(tiles)], 0
    )
    first = lax.broadcasted_iota(jnp.int32, (LANES, LANES), 0)
    second = lax.broadcasted_iota(jnp.int32, (LANES, LANES), 1)
    counts = dot(as_bf16(stacked), as_bf16(jnp.where(first <= second, 1.0, 0.0)))
    places = []
    for side in range(2):
        base = jnp.zeros((1, 1), jnp.float32)
        line = []
        for t in range(tiles):
            row = counts[side * tiles + t : side * tiles + t + 1]
            line.append(row + base)
            base = base + row[:, LANES - 1 :]
        places.append(jnp.concatenate(line, 1).astype(jnp.int32) - 1)
    place = jnp.where(leaving[0], places[0], jnp.where(leaving[1], MOVE + places[1], -1))
    chosen = one_hot(place, 2 * MOVE)
    out = dot_rows(chosen, jnp.concatenate(parts_of(payload[...], 3), 0))
    packed = out[:, :ROWS] + (out[:, ROWS : 2 * ROWS] + out[:, 2 * ROWS :])
    left_ref[...] = packed[:MOVE]
    right_ref[...] = packed[MOVE:]


def stay_kernel(rhs_ref, cond_ref, dest_ref, placed_ref, payload):
    cells = dest_ref.shape[1]
    target, slot = targets(dest_ref)
    fill_payload(payload, rhs_ref, cond_ref, slot)
    chosen = one_hot(jnp.where(target == 0, slot, -1), cells)
    out = dot_rows(jnp.concatenate(parts_of(payload[...], 3), 0), chosen)
    placed_ref[...] = out[:ROWS] + (out[ROWS : 2 * ROWS] + out[2 * ROWS :])


def face_traces(field, kappa, trace_ref, send_ref, data_ref, left_ref, right_ref):
    cells = field.shape[1]
    out = times3(trace_ref[...], field)
    row = lax.broadcasted_iota(jnp.int32, (HALF, 1), 0)
    for face in range(FACES):
        start = face * SLAB
        values = jnp.where(row == FACE, kappa, out[start : start + HALF])
        data_ref[start : start + HALF] = values
        data_ref[start + HALF : start + SLAB] = kappa * out[start + HALF : start + SLAB]
    data_ref[FACES * SLAB :] = kappa * out[FACES * SLAB :]
    for face, ref in ((0, left_ref), (1, right_ref)):
        chosen = one_hot(send_ref[face : face + 1], cells)
        ref[...] = pick(data_ref[face * SLAB : (face + 1) * SLAB], chosen, 2)


def arrive_kernel(placed_ref, from_left_ref, from_right_ref, trace_ref, send_ref,
                  field_ref, kappa_ref, data_ref, left_ref, right_ref):
    cells = placed_ref.shape[1]
    records = jnp.concatenate([from_left_ref[...], from_right_ref[...]], 0)
    slot = records[:, BLOCK + 1 : BLOCK + 2].astype(jnp.int32) - 1
    ids = lax.broadcasted_iota(jnp.int32, (2 * MOVE, cells), 1)
    chosen = as_bf16(jnp.where(ids == slot, 1.0, 0.0))
    merged = placed_ref[...] + pick(records.T, chosen, 3)
    kappa = merged[BLOCK : BLOCK + 1]
    row = lax.broadcasted_iota(jnp.int32, (ROWS, 1), 0)
    field = jnp.where(row < BLOCK, merged, 0.0)
    field_ref[...] = field
    kappa_ref[...] = kappa
    face_traces(field, kappa, trace_ref, send_ref, data_ref, left_ref, right_ref)


def face_terms(face, near, own, kappa, neighbour_ref, code_ref, flips):
    code = code_ref[face : face + 1]
    first = as_f32(jnp.bitwise_and(code, 1))
    second = as_f32(jnp.right_shift(code, 1))
    sign = (1.0 - 2.0 * first * flips[:, 0:1]) * (1.0 - 2.0 * second * flips[:, 1:2])
    outside = jnp.where(neighbour_ref[face : face + 1] < 0, 2.0, 1.0)
    jump = outside * own - sign * near
    strength = PENALTY * jnp.maximum(kappa, near[FACE : FACE + 1])
    values, fluxes = jump[:HALF], jump[HALF:]
    return jnp.concatenate([strength * values - 0.5 * fluxes, kappa * values], 0)


def local_kernel(field_ref, kappa_ref, data_ref, neighbour_ref, code_ref, back_ref, weight_ref, flip_ref,
                 part_ref, near_ref):
    cells = field_ref.shape[1]
    kappa = kappa_ref[...]
    flips = flip_ref[...]
    terms = []
    for face in range(FACES):
        other = (face ^ 1) * SLAB
        chosen = one_hot(neighbour_ref[face : face + 1], cells)
        near = pick(data_ref[other : other + SLAB], chosen, 2)
        if face < 2:
            near_ref[face * SLAB : (face + 1) * SLAB] = near
        else:
            own = data_ref[face * SLAB : (face + 1) * SLAB]
            terms.append(face_terms(face, near, own, kappa, neighbour_ref, code_ref, flips))
    volume = weight_ref[...] * field_ref[...] + data_ref[FACES * SLAB :]
    part_ref[...] = volume + times3(back_ref[...], jnp.concatenate(terms, 0))


def finish(part_ref, near_ref, data_ref, kappa, from_left_ref, from_right_ref, neighbour_ref, code_ref,
           back_ref, flip_ref):
    cells = part_ref.shape[1]
    flips = flip_ref[...]
    terms = []
    for face, ghost_ref in ((0, from_left_ref), (1, from_right_ref)):
        ghosts = ghost_ref.shape[1]
        chosen = one_hot(neighbour_ref[face : face + 1], ghosts, cells + face * ghosts)
        near = near_ref[face * SLAB : (face + 1) * SLAB] + pick(ghost_ref[...], chosen, 2)
        own = data_ref[face * SLAB : (face + 1) * SLAB]
        terms.append(face_terms(face, near, own, kappa, neighbour_ref, code_ref, flips))
    return part_ref[...] + times3(back_ref[...], jnp.concatenate(terms, 0))


def middle_kernel(part_ref, near_ref, data_ref, kappa_ref, from_left_ref, from_right_ref, neighbour_ref,
                  code_ref, back_ref, flip_ref, trace_ref, send_ref,
                  image_ref, next_ref, left_ref, right_ref):
    kappa = kappa_ref[...]
    image = finish(part_ref, near_ref, data_ref, kappa, from_left_ref, from_right_ref, neighbour_ref,
                   code_ref, back_ref, flip_ref)
    image_ref[...] = image
    face_traces(image, kappa, trace_ref, send_ref, next_ref, left_ref, right_ref)


def last_kernel(part_ref, near_ref, data_ref, kappa_ref, from_left_ref, from_right_ref, neighbour_ref,
                code_ref, back_ref, flip_ref, field_ref, image_ref, twice_ref, sums_ref):
    twice = finish(part_ref, near_ref, data_ref, kappa_ref[...], from_left_ref, from_right_ref, neighbour_ref,
                   code_ref, back_ref, flip_ref)
    twice_ref[...] = twice
    field, image = field_ref[...], image_ref[...]
    lane = lax.broadcasted_iota(jnp.int32, (1, LANES), 1)
    sums = jnp.zeros((1, LANES), jnp.float32)
    pairs = ((field, field), (field, image), (image, image), (field, twice), (image, twice))
    for place, (one, two) in enumerate(pairs):
        column = jnp.sum(one * two, axis=0, keepdims=True)
        total = jnp.sum(column, axis=1, keepdims=True)
        sums = jnp.where(lane == place, total, sums)
    sums_ref[...] = sums


def update_kernel(sums_ref, field_ref, image_ref, twice_ref, solution_ref, residual_ref):
    sums = sums_ref[...]
    bb, bw, ww, bt, wt = (sums[:, place : place + 1] for place in range(5))
    alpha = bb / bw
    rr = bb - 2.0 * alpha * bw + alpha * alpha * ww
    beta = rr / bb
    more = 1.0 + beta
    inner = more * more * bw - alpha * more * (bt + ww) + alpha * alpha * wt
    step = rr / inner
    field, image, twice = field_ref[:BLOCK], image_ref[:BLOCK], twice_ref[:BLOCK]
    direction = more * field - alpha * image
    along = more * image - alpha * twice
    solution_ref[...] = alpha * field + step * direction
    residual_ref[...] = (field - alpha * image) - step * along


def exchange(to_left, to_right):
    count = lax.axis_size(AXES)
    forward = [(i, i + 1) for i in range(count - 1)]
    backward = [(i + 1, i) for i in range(count - 1)]
    return lax.ppermute(to_right, AXES, forward), lax.ppermute(to_left, AXES, backward)


def sum_all(value):
    for axis in AXES:
        size = lax.axis_size(axis)
        if size & (size - 1):
            value = lax.psum(value, axis)
            continue
        bit = 1
        while bit < size:
            value = value + lax.ppermute(value, axis, [(i, i ^ bit) for i in range(size)])
            bit *= 2
    return value


def body(right_side, conductivity, destination, neighbour, orientation, send_list):
    trace3, back_ghost, back_local, weight_rows, flips = (jnp.asarray(t) for t in operator_constants())
    cells = destination.shape[0]
    ghosts = send_list.shape[1]
    cond = conductivity[None]
    dest = destination[None]
    big = 2 * ROWS * cells
    payload = pltpu.VMEM((ROWS, cells), jnp.float32)
    left, right = call(pack_kernel, [f32(MOVE, ROWS)] * 2, [right_side, cond, dest],
                       big * LANES * 3, [payload], "pack")
    from_left, from_right = exchange(left, right)
    (placed,) = call(stay_kernel, [f32(ROWS, cells)], [right_side, cond, dest],
                     big * cells * 3, [payload], "stay")
    trace_outs = [f32(FACES * SLAB + ROWS, cells), f32(SLAB, ghosts), f32(SLAB, ghosts)]
    trace_flops = big * (FACES * SLAB + ROWS) * 3
    field, kappa, data, left, right = call(
        arrive_kernel, [f32(ROWS, cells), f32(1, cells)] + trace_outs,
        [placed, from_left, from_right, trace3, send_list], trace_flops, (), "arrive")

    def local(vector, data):
        return call(local_kernel, [f32(ROWS, cells), f32(2 * SLAB, cells)],
                    [vector, kappa, data, neighbour, orientation, back_local, weight_rows, flips],
                    big * cells * FACES * 2, (), "local")

    from_left, from_right = exchange(left, right)
    part, near = local(field, data)
    image, data, left, right = call(
        middle_kernel, [f32(ROWS, cells)] + trace_outs,
        [part, near, data, kappa, from_left, from_right, neighbour, orientation, back_ghost, flips,
         trace3, send_list], trace_flops, (), "middle")
    from_left, from_right = exchange(left, right)
    part, near = local(image, data)
    twice, sums = call(
        last_kernel, [f32(ROWS, cells), f32(1, LANES)],
        [part, near, data, kappa, from_left, from_right, neighbour, orientation, back_ghost, flips,
         field, image], big * 2 * SLAB * 3, (), "last")
    sums = sum_all(sums)
    return tuple(call(update_kernel, [f32(BLOCK, cells)] * 2, [sums, field, image, twice],
                      big, (), "update"))


def solution(mesh):
    in_specs = (
        P(None, AXES),
        P(AXES),
        P(AXES),
        P(None, AXES),
        P(None, AXES),
        P(None, AXES),
    )
    out_specs = (P(None, AXES), P(None, AXES))
    return jax.shard_map(body, mesh=mesh, in_specs=in_specs, out_specs=out_specs, check_vma=False)
```

```python
import functools

import jax
import jax.numpy as jnp
import numpy as np
from jax import lax
from jax.experimental import pallas as pl
from jax.experimental.pallas import tpu as pltpu
from jax.sharding import PartitionSpec as P

NODES = 5
FACE = NODES * NODES
BLOCK = NODES**3
MOVE = 64
LANES = 128
ROWS = 128
HALF = 32
SLAB = 2 * HALF
FACES = 6
PENALTY = 80.0
AXES = ("curve", "group")
VMEM_LIMIT = 24 * 1024 * 1024

GAUSS_POINTS = (-0.906179845938664, -0.5384693101056831, 0.0, 0.5384693101056831, 0.906179845938664)
GAUSS_WEIGHTS = (
    0.2369268850561891,
    0.4786286704993665,
    0.5688888888888889,
    0.4786286704993665,
    0.2369268850561891,
)


def lagrange_value(points, position, location):
    value = 1.0
    for other in range(len(points)):
        if other != position:
            value = value * (location - points[other]) / (points[position] - points[other])
    return value


def lagrange_slope(points, position, location):
    total = 0.0
    for skipped in range(len(points)):
        if skipped == position:
            continue
        addend = 1.0 / (points[position] - points[skipped])
        for other in range(len(points)):
            if other != position and other != skipped:
                addend = addend * (location - points[other]) / (points[position] - points[other])
        total = total + addend
    return total


def basis_tables():
    points = [0.5 * (value + 1.0) for value in GAUSS_POINTS]
    weights = [0.5 * value for value in GAUSS_WEIGHTS]
    count = len(points)
    slopes = [[lagrange_slope(points, p, points[q]) for p in range(count)] for q in range(count)]
    start_value = [lagrange_value(points, p, 0.0) for p in range(count)]
    end_value = [lagrange_value(points, p, 1.0) for p in range(count)]
    start_slope = [-lagrange_slope(points, p, 0.0) for p in range(count)]
    end_slope = [lagrange_slope(points, p, 1.0) for p in range(count)]
    listed = (weights, slopes, start_value, end_value, start_slope, end_slope)
    return [np.asarray(np.asarray(table, np.float32), np.float64) for table in listed]


def along_axis(matrix, axis_id):
    factors = [np.eye(NODES)] * 3
    factors[axis_id] = matrix
    return np.kron(factors[0], np.kron(factors[1], factors[2]))


def parity_basis():
    root = np.sqrt(0.5)
    line = np.zeros((NODES, NODES))
    line[0, 0] = line[0, 4] = line[1, 1] = line[1, 3] = root
    line[2, 2] = 1.0
    line[3, 0], line[3, 4] = root, -root
    line[4, 1], line[4, 3] = root, -root
    odd = np.array([0, 0, 0, 1, 1])
    return np.kron(line, line), np.repeat(odd, NODES), np.tile(odd, NODES)


def split_two(matrix):
    high = matrix.astype(np.float32).astype(jnp.bfloat16)
    low = (matrix - high.astype(np.float64)).astype(np.float32).astype(jnp.bfloat16)
    return high, low


@functools.cache
def operator_constants():
    weights, slopes, *ends = basis_tables()
    cell_weight = np.kron(weights, np.kron(weights, weights))
    face_weight = np.kron(weights, weights)
    parity, odd_first, odd_second = parity_basis()
    stiff = np.zeros((BLOCK, BLOCK))
    for axis_id in range(3):
        grad = along_axis(slopes, axis_id)
        stiff += grad.T @ (cell_weight[:, None] * grad)
    trace = np.zeros((FACES * SLAB + ROWS, ROWS))
    back = np.zeros((ROWS, FACES * SLAB))
    for face in range(FACES):
        tangent = along_axis(ends[face % 2][None, :], face // 2)
        normal = along_axis(ends[2 + face % 2][None, :], face // 2)
        start = face * SLAB
        trace[start : start + FACE, :BLOCK] = parity @ tangent
        trace[start + HALF : start + HALF + FACE, :BLOCK] = parity @ normal
        spread = (face_weight[:, None] * parity.T)
        back[:BLOCK, start : start + FACE] = tangent.T @ spread
        back[:BLOCK, start + HALF : start + HALF + FACE] = -0.5 * normal.T @ spread
    trace[FACES * SLAB : FACES * SLAB + BLOCK, :BLOCK] = stiff
    high, low = split_two(trace)
    trace3 = np.concatenate([high, high, low], 1)
    backs = []
    for first, last in ((0, 2), (2, FACES)):
        high, low = split_two(back[:, first * SLAB : last * SLAB])
        backs.append(np.concatenate([high, high, low], 1))
    weight_rows = np.zeros((ROWS, 1), np.float32)
    weight_rows[:BLOCK, 0] = cell_weight
    flips = np.zeros((SLAB, LANES), np.float32)
    for start in (0, HALF):
        flips[start : start + FACE, 0] = odd_first
        flips[start : start + FACE, 1] = odd_second
    return trace3, backs[0], backs[1], weight_rows, flips


def as_bf16(value):
    return value.astype(jnp.bfloat16)


def as_f32(value):
    return value.astype(jnp.float32)


def parts_of(value, count):
    pieces = []
    for step in range(count):
        piece = as_bf16(value)
        pieces.append(piece)
        if step + 1 < count:
            value = value - as_f32(piece)
    return pieces


def dot(left, right):
    return lax.dot_general(left, right, (((1,), (0,)), ((), ())), preferred_element_type=jnp.float32)


def dot_rows(left, right):
    return lax.dot_general(left, right, (((1,), (1,)), ((), ())), preferred_element_type=jnp.float32)


def times3(table3, value):
    high, low = parts_of(value, 2)
    return dot(table3, jnp.concatenate([high, low, high], 0))


def pick(value, chosen, count):
    rows = value.shape[0]
    out = dot(jnp.concatenate(parts_of(value, count), 0), chosen)
    total = out[(count - 1) * rows :]
    for step in reversed(range(count - 1)):
        total = total + out[step * rows : (step + 1) * rows]
    return total


def one_hot(index_row, rows, offset=0):
    ids = lax.broadcasted_iota(jnp.int32, (rows, index_row.shape[1]), 0)
    return as_bf16(jnp.where(ids == index_row - offset, 1.0, 0.0))


def whole(ref_list):
    return [pl.BlockSpec(memory_space=pltpu.VMEM) for _ in ref_list]


def call(kernel, outs, args, flops, scratch=(), name=None):
    moved = sum(a.size * a.dtype.itemsize for a in args) + sum(o.size * o.dtype.itemsize for o in outs)
    return pl.pallas_call(
        kernel,
        out_shape=list(outs),
        in_specs=whole(args),
        out_specs=whole(outs),
        scratch_shapes=list(scratch),
        compiler_params=pltpu.CompilerParams(vmem_limit_bytes=VMEM_LIMIT),
        cost_estimate=pl.CostEstimate(flops=flops, bytes_accessed=moved, transcendentals=0),
        name=name,
    )(*args)


def f32(*shape):
    return jax.ShapeDtypeStruct(shape, jnp.float32)


def targets(dest_ref):
    cells = dest_ref.shape[1]
    rank = lax.axis_index("curve") * lax.axis_size("group") + lax.axis_index("group")
    dest = dest_ref[...]
    owner = lax.div(dest, cells)
    return owner - rank, dest - owner * cells


def fill_payload(payload, rhs_ref, cond_ref, slot):
    payload[:BLOCK] = rhs_ref[...]
    payload[BLOCK : BLOCK + 1] = cond_ref[...]
    payload[BLOCK + 1 : BLOCK + 2] = as_f32(slot + 1)
    payload[BLOCK + 2 : ROWS] = jnp.zeros((ROWS - BLOCK - 2, payload.shape[1]), jnp.float32)


def pack_kernel(rhs_ref, cond_ref, dest_ref, left_ref, right_ref, payload):
    cells = dest_ref.shape[1]
    tiles = cells // LANES
    target, slot = targets(dest_ref)
    fill_payload(payload, rhs_ref, cond_ref, slot)
    leaving = [target == -1, target == 1]
    marks = [as_f32(mask) for mask in leaving]
    stacked = jnp.concatenate(
        [mark[:, t * LANES : (t + 1) * LANES] for mark in marks for t in range(tiles)], 0
    )
    first = lax.broadcasted_iota(jnp.int32, (LANES, LANES), 0)
    second = lax.broadcasted_iota(jnp.int32, (LANES, LANES), 1)
    counts = dot(as_bf16(stacked), as_bf16(jnp.where(first <= second, 1.0, 0.0)))
    places = []
    for side in range(2):
        base = jnp.zeros((1, 1), jnp.float32)
        line = []
        for t in range(tiles):
            row = counts[side * tiles + t : side * tiles + t + 1]
            line.append(row + base)
            base = base + row[:, LANES - 1 :]
        places.append(jnp.concatenate(line, 1).astype(jnp.int32) - 1)
    place = jnp.where(leaving[0], places[0], jnp.where(leaving[1], MOVE + places[1], -1))
    chosen = one_hot(place, 2 * MOVE)
    out = dot_rows(chosen, jnp.concatenate(parts_of(payload[...], 3), 0))
    packed = out[:, :ROWS] + (out[:, ROWS : 2 * ROWS] + out[:, 2 * ROWS :])
    left_ref[...] = packed[:MOVE]
    right_ref[...] = packed[MOVE:]


def stay_kernel(rhs_ref, cond_ref, dest_ref, placed_ref, payload):
    cells = dest_ref.shape[1]
    target, slot = targets(dest_ref)
    fill_payload(payload, rhs_ref, cond_ref, slot)
    chosen = one_hot(jnp.where(target == 0, slot, -1), cells)
    out = dot_rows(jnp.concatenate(parts_of(payload[...], 3), 0), chosen)
    placed_ref[...] = out[:ROWS] + (out[ROWS : 2 * ROWS] + out[2 * ROWS :])


def face_traces(field, kappa, trace_ref, send_ref, data_ref, left_ref, right_ref):
    cells = field.shape[1]
    out = times3(trace_ref[...], field)
    row = lax.broadcasted_iota(jnp.int32, (HALF, 1), 0)
    for face in range(FACES):
        start = face * SLAB
        values = jnp.where(row == FACE, kappa, out[start : start + HALF])
        data_ref[start : start + HALF] = values
        data_ref[start + HALF : start + SLAB] = kappa * out[start + HALF : start + SLAB]
    data_ref[FACES * SLAB :] = kappa * out[FACES * SLAB :]
    for face, ref in ((0, left_ref), (1, right_ref)):
        chosen = one_hot(send_ref[face : face + 1], cells)
        ref[...] = pick(data_ref[face * SLAB : (face + 1) * SLAB], chosen, 2)


def arrive_kernel(placed_ref, from_left_ref, from_right_ref, trace_ref, send_ref,
                  field_ref, kappa_ref, data_ref, left_ref, right_ref):
    cells = placed_ref.shape[1]
    records = jnp.concatenate([from_left_ref[...], from_right_ref[...]], 0)
    slot = records[:, BLOCK + 1 : BLOCK + 2].astype(jnp.int32) - 1
    ids = lax.broadcasted_iota(jnp.int32, (2 * MOVE, cells), 1)
    chosen = as_bf16(jnp.where(ids == slot, 1.0, 0.0))
    merged = placed_ref[...] + pick(records.T, chosen, 3)
    kappa = merged[BLOCK : BLOCK + 1]
    row = lax.broadcasted_iota(jnp.int32, (ROWS, 1), 0)
    field = jnp.where(row < BLOCK, merged, 0.0)
    field_ref[...] = field
    kappa_ref[...] = kappa
    face_traces(field, kappa, trace_ref, send_ref, data_ref, left_ref, right_ref)


def face_terms(face, near, own, kappa, neighbour_ref, code_ref, flips):
    code = code_ref[face : face + 1]
    first = as_f32(jnp.bitwise_and(code, 1))
    second = as_f32(jnp.right_shift(code, 1))
    sign = (1.0 - 2.0 * first * flips[:, 0:1]) * (1.0 - 2.0 * second * flips[:, 1:2])
    outside = jnp.where(neighbour_ref[face : face + 1] < 0, 2.0, 1.0)
    jump = outside * own - sign * near
    strength = PENALTY * jnp.maximum(kappa, near[FACE : FACE + 1])
    values, fluxes = jump[:HALF], jump[HALF:]
    return jnp.concatenate([strength * values - 0.5 * fluxes, kappa * values], 0)


def local_kernel(field_ref, kappa_ref, data_ref, neighbour_ref, code_ref, back_ref, weight_ref, flip_ref,
                 part_ref, near_ref):
    cells = field_ref.shape[1]
    kappa = kappa_ref[...]
    flips = flip_ref[...]
    terms = []
    for face in range(FACES):
        other = (face ^ 1) * SLAB
        chosen = one_hot(neighbour_ref[face : face + 1], cells)
        near = pick(data_ref[other : other + SLAB], chosen, 2)
        if face < 2:
            near_ref[face * SLAB : (face + 1) * SLAB] = near
        else:
            own = data_ref[face * SLAB : (face + 1) * SLAB]
            terms.append(face_terms(face, near, own, kappa, neighbour_ref, code_ref, flips))
    volume = weight_ref[...] * field_ref[...] + data_ref[FACES * SLAB :]
    part_ref[...] = volume + times3(back_ref[...], jnp.concatenate(terms, 0))


def finish(part_ref, near_ref, data_ref, kappa, from_left_ref, from_right_ref, neighbour_ref, code_ref,
           back_ref, flip_ref):
    cells = part_ref.shape[1]
    flips = flip_ref[...]
    terms = []
    for face, ghost_ref in ((0, from_left_ref), (1, from_right_ref)):
        ghosts = ghost_ref.shape[1]
        chosen = one_hot(neighbour_ref[face : face + 1], ghosts, cells + face * ghosts)
        near = near_ref[face * SLAB : (face + 1) * SLAB] + pick(ghost_ref[...], chosen, 2)
        own = data_ref[face * SLAB : (face + 1) * SLAB]
        terms.append(face_terms(face, near, own, kappa, neighbour_ref, code_ref, flips))
    return part_ref[...] + times3(back_ref[...], jnp.concatenate(terms, 0))


def middle_kernel(part_ref, near_ref, data_ref, kappa_ref, from_left_ref, from_right_ref, neighbour_ref,
                  code_ref, back_ref, flip_ref, trace_ref, send_ref,
                  image_ref, next_ref, left_ref, right_ref):
    kappa = kappa_ref[...]
    image = finish(part_ref, near_ref, data_ref, kappa, from_left_ref, from_right_ref, neighbour_ref,
                   code_ref, back_ref, flip_ref)
    image_ref[...] = image
    face_traces(image, kappa, trace_ref, send_ref, next_ref, left_ref, right_ref)


def last_kernel(part_ref, near_ref, data_ref, kappa_ref, from_left_ref, from_right_ref, neighbour_ref,
                code_ref, back_ref, flip_ref, field_ref, image_ref, twice_ref, sums_ref):
    twice = finish(part_ref, near_ref, data_ref, kappa_ref[...], from_left_ref, from_right_ref, neighbour_ref,
                   code_ref, back_ref, flip_ref)
    twice_ref[...] = twice
    field, image = field_ref[...], image_ref[...]
    lane = lax.broadcasted_iota(jnp.int32, (1, LANES), 1)
    sums = jnp.zeros((1, LANES), jnp.float32)
    pairs = ((field, field), (field, image), (image, image), (field, twice), (image, twice))
    for place, (one, two) in enumerate(pairs):
        column = jnp.sum(one * two, axis=0, keepdims=True)
        total = jnp.sum(column, axis=1, keepdims=True)
        sums = jnp.where(lane == place, total, sums)
    sums_ref[...] = jnp.broadcast_to(sums, sums_ref.shape)


def update_kernel(sums_ref, field_ref, image_ref, twice_ref, solution_ref, residual_ref):
    sums = jnp.sum(sums_ref[...], axis=0, keepdims=True)
    bb, bw, ww, bt, wt = (sums[:, place : place + 1] for place in range(5))
    alpha = bb / bw
    rr = bb - 2.0 * alpha * bw + alpha * alpha * ww
    beta = rr / bb
    more = 1.0 + beta
    inner = more * more * bw - alpha * more * (bt + ww) + alpha * alpha * wt
    step = rr / inner
    field, image, twice = field_ref[:BLOCK], image_ref[:BLOCK], twice_ref[:BLOCK]
    direction = more * field - alpha * image
    along = more * image - alpha * twice
    solution_ref[...] = alpha * field + step * direction
    residual_ref[...] = (field - alpha * image) - step * along


def exchange(to_left, to_right):
    count = lax.axis_size(AXES)
    forward = [(i, (i + 1) % count) for i in range(count)]
    backward = [((i + 1) % count, i) for i in range(count)]
    return lax.ppermute(to_right, AXES, forward), lax.ppermute(to_left, AXES, backward)


def body(right_side, conductivity, destination, neighbour, orientation, send_list):
    trace3, back_ghost, back_local, weight_rows, flips = (jnp.asarray(t) for t in operator_constants())
    cells = destination.shape[0]
    ghosts = send_list.shape[1]
    cond = conductivity[None]
    dest = destination[None]
    big = 2 * ROWS * cells
    payload = pltpu.VMEM((ROWS, cells), jnp.float32)
    left, right = call(pack_kernel, [f32(MOVE, ROWS)] * 2, [right_side, cond, dest],
                       big * LANES * 3, [payload], "pack")
    from_left, from_right = exchange(left, right)
    (placed,) = call(stay_kernel, [f32(ROWS, cells)], [right_side, cond, dest],
                     big * cells * 3, [payload], "stay")
    trace_outs = [f32(FACES * SLAB + ROWS, cells), f32(SLAB, ghosts), f32(SLAB, ghosts)]
    trace_flops = big * (FACES * SLAB + ROWS) * 3
    field, kappa, data, left, right = call(
        arrive_kernel, [f32(ROWS, cells), f32(1, cells)] + trace_outs,
        [placed, from_left, from_right, trace3, send_list], trace_flops, (), "arrive")

    def local(vector, data):
        return call(local_kernel, [f32(ROWS, cells), f32(2 * SLAB, cells)],
                    [vector, kappa, data, neighbour, orientation, back_local, weight_rows, flips],
                    big * cells * FACES * 2, (), "local")

    from_left, from_right = exchange(left, right)
    part, near = local(field, data)
    image, data, left, right = call(
        middle_kernel, [f32(ROWS, cells)] + trace_outs,
        [part, near, data, kappa, from_left, from_right, neighbour, orientation, back_ghost, flips,
         trace3, send_list], trace_flops, (), "middle")
    from_left, from_right = exchange(left, right)
    part, near = local(image, data)
    twice, sums = call(
        last_kernel, [f32(ROWS, cells), f32(lax.axis_size(AXES), LANES)],
        [part, near, data, kappa, from_left, from_right, neighbour, orientation, back_ghost, flips,
         field, image], big * 2 * SLAB * 3, (), "last")
    sums = lax.all_to_all(sums, AXES, 0, 0, tiled=True)
    return tuple(call(update_kernel, [f32(BLOCK, cells)] * 2, [sums, field, image, twice],
                      big, (), "update"))


def solution(mesh):
    in_specs = (
        P(None, AXES),
        P(AXES),
        P(AXES),
        P(None, AXES),
        P(None, AXES),
        P(None, AXES),
    )
    out_specs = (P(None, AXES), P(None, AXES))
    return jax.shard_map(body, mesh=mesh, in_specs=in_specs, out_specs=out_specs, check_vma=False)
```

```python
import functools

import jax
import jax.numpy as jnp
import numpy as np
from jax import lax
from jax.experimental import pallas as pl
from jax.experimental.pallas import tpu as pltpu
from jax.sharding import PartitionSpec as P

NODES = 5
FACE = NODES * NODES
BLOCK = NODES**3
MOVE = 64
LANES = 128
ROWS = 128
HALF = 32
SLAB = 2 * HALF
FACES = 6
PENALTY = 80.0
AXES = ("curve", "group")
VMEM_LIMIT = 24 * 1024 * 1024

GAUSS_POINTS = (-0.906179845938664, -0.5384693101056831, 0.0, 0.5384693101056831, 0.906179845938664)
GAUSS_WEIGHTS = (
    0.2369268850561891,
    0.4786286704993665,
    0.5688888888888889,
    0.4786286704993665,
    0.2369268850561891,
)


def lagrange_value(points, position, location):
    value = 1.0
    for other in range(len(points)):
        if other != position:
            value = value * (location - points[other]) / (points[position] - points[other])
    return value


def lagrange_slope(points, position, location):
    total = 0.0
    for skipped in range(len(points)):
        if skipped == position:
            continue
        addend = 1.0 / (points[position] - points[skipped])
        for other in range(len(points)):
            if other != position and other != skipped:
                addend = addend * (location - points[other]) / (points[position] - points[other])
        total = total + addend
    return total


def basis_tables():
    points = [0.5 * (value + 1.0) for value in GAUSS_POINTS]
    weights = [0.5 * value for value in GAUSS_WEIGHTS]
    count = len(points)
    slopes = [[lagrange_slope(points, p, points[q]) for p in range(count)] for q in range(count)]
    start_value = [lagrange_value(points, p, 0.0) for p in range(count)]
    end_value = [lagrange_value(points, p, 1.0) for p in range(count)]
    start_slope = [-lagrange_slope(points, p, 0.0) for p in range(count)]
    end_slope = [lagrange_slope(points, p, 1.0) for p in range(count)]
    listed = (weights, slopes, start_value, end_value, start_slope, end_slope)
    return [np.asarray(np.asarray(table, np.float32), np.float64) for table in listed]


def along_axis(matrix, axis_id):
    factors = [np.eye(NODES)] * 3
    factors[axis_id] = matrix
    return np.kron(factors[0], np.kron(factors[1], factors[2]))


def parity_basis():
    root = np.sqrt(0.5)
    line = np.zeros((NODES, NODES))
    line[0, 0] = line[0, 4] = line[1, 1] = line[1, 3] = root
    line[2, 2] = 1.0
    line[3, 0], line[3, 4] = root, -root
    line[4, 1], line[4, 3] = root, -root
    odd = np.array([0, 0, 0, 1, 1])
    return np.kron(line, line), np.repeat(odd, NODES), np.tile(odd, NODES)


def split_two(matrix):
    high = matrix.astype(np.float32).astype(jnp.bfloat16)
    low = (matrix - high.astype(np.float64)).astype(np.float32).astype(jnp.bfloat16)
    return high, low


@functools.cache
def operator_constants():
    weights, slopes, *ends = basis_tables()
    cell_weight = np.kron(weights, np.kron(weights, weights))
    face_weight = np.kron(weights, weights)
    parity, odd_first, odd_second = parity_basis()
    stiff = np.zeros((BLOCK, BLOCK))
    for axis_id in range(3):
        grad = along_axis(slopes, axis_id)
        stiff += grad.T @ (cell_weight[:, None] * grad)
    trace = np.zeros((FACES * SLAB + ROWS, ROWS))
    back = np.zeros((ROWS, FACES * SLAB))
    for face in range(FACES):
        tangent = along_axis(ends[face % 2][None, :], face // 2)
        normal = along_axis(ends[2 + face % 2][None, :], face // 2)
        start = face * SLAB
        trace[start : start + FACE, :BLOCK] = parity @ tangent
        trace[start + HALF : start + HALF + FACE, :BLOCK] = parity @ normal
        spread = (face_weight[:, None] * parity.T)
        back[:BLOCK, start : start + FACE] = tangent.T @ spread
        back[:BLOCK, start + HALF : start + HALF + FACE] = -0.5 * normal.T @ spread
    trace[FACES * SLAB : FACES * SLAB + BLOCK, :BLOCK] = stiff
    high, low = split_two(trace)
    trace3 = np.concatenate([high, high, low], 1)
    trace_pair, trace_rest = trace3[: 2 * SLAB], trace3[2 * SLAB :]
    backs = []
    for first, last in ((0, 2), (2, FACES)):
        high, low = split_two(back[:, first * SLAB : last * SLAB])
        backs.append(np.concatenate([high, high, low], 1))
    weight_rows = np.zeros((ROWS, 1), np.float32)
    weight_rows[:BLOCK, 0] = cell_weight
    flips = np.zeros((SLAB, LANES), np.float32)
    for start in (0, HALF):
        flips[start : start + FACE, 0] = odd_first
        flips[start : start + FACE, 1] = odd_second
        flips[start : start + FACE, 2] = np.diag(parity @ (face_weight[:, None] * parity.T))
    return trace_pair, trace_rest, backs[0], backs[1], weight_rows, flips


def as_bf16(value):
    return value.astype(jnp.bfloat16)


def as_f32(value):
    return value.astype(jnp.float32)


def parts_of(value, count):
    pieces = []
    for step in range(count):
        piece = as_bf16(value)
        pieces.append(piece)
        if step + 1 < count:
            value = value - as_f32(piece)
    return pieces


def dot(left, right):
    return lax.dot_general(left, right, (((1,), (0,)), ((), ())), preferred_element_type=jnp.float32)


def dot_rows(left, right):
    return lax.dot_general(left, right, (((1,), (1,)), ((), ())), preferred_element_type=jnp.float32)


def times3(table3, value):
    high, low = parts_of(value, 2)
    return dot(table3, jnp.concatenate([high, low, high], 0))


def pick(value, chosen, count):
    rows = value.shape[0]
    out = dot(jnp.concatenate(parts_of(value, count), 0), chosen)
    total = out[(count - 1) * rows :]
    for step in reversed(range(count - 1)):
        total = total + out[step * rows : (step + 1) * rows]
    return total


def one_hot(index_row, rows, offset=0):
    ids = lax.broadcasted_iota(jnp.int32, (rows, index_row.shape[1]), 0)
    return as_bf16(jnp.where(ids == index_row - offset, 1.0, 0.0))


def call(kernel, outs, args, flops, scratch=(), name=None, far=0):
    moved = sum(a.size * a.dtype.itemsize for a in args) + sum(o.size * o.dtype.itemsize for o in outs)
    spaces = [pltpu.MemorySpace.HBM] * far + [pltpu.VMEM] * (len(args) - far)
    return pl.pallas_call(
        kernel,
        out_shape=list(outs),
        in_specs=[pl.BlockSpec(memory_space=space) for space in spaces],
        out_specs=[pl.BlockSpec(memory_space=pltpu.VMEM) for _ in outs],
        scratch_shapes=list(scratch),
        compiler_params=pltpu.CompilerParams(vmem_limit_bytes=VMEM_LIMIT),
        cost_estimate=pl.CostEstimate(flops=flops, bytes_accessed=moved, transcendentals=0),
        name=name,
    )(*args)


def f32(*shape):
    return jax.ShapeDtypeStruct(shape, jnp.float32)


def pack_kernel(rhs_hbm, cond_hbm, dest_hbm, left_ref, right_ref, payload_ref, stay_ref, rhs, cond, dest_row, sems):
    cells = dest_row.shape[1]
    tiles = cells // LANES
    copies = [
        pltpu.make_async_copy(dest_hbm, dest_row, sems.at[0]),
        pltpu.make_async_copy(cond_hbm, cond, sems.at[1]),
        pltpu.make_async_copy(rhs_hbm, rhs, sems.at[2]),
    ]
    for copy in copies:
        copy.start()
    copies[0].wait()
    rank = lax.axis_index("curve") * lax.axis_size("group") + lax.axis_index("group")
    dest = dest_row[...]
    owner = lax.div(dest, cells)
    target, slot = owner - rank, dest - owner * cells
    stay_ref[...] = jnp.where(target == 0, slot, -1)
    leaving = [target == -1, target == 1]
    marks = [as_f32(mask) for mask in leaving]
    stacked = jnp.concatenate(
        [mark[:, t * LANES : (t + 1) * LANES] for mark in marks for t in range(tiles)], 0
    )
    first = lax.broadcasted_iota(jnp.int32, (LANES, LANES), 0)
    second = lax.broadcasted_iota(jnp.int32, (LANES, LANES), 1)
    counts = dot(as_bf16(stacked), as_bf16(jnp.where(first <= second, 1.0, 0.0)))
    places = []
    for side in range(2):
        base = jnp.zeros((1, 1), jnp.float32)
        line = []
        for t in range(tiles):
            row = counts[side * tiles + t : side * tiles + t + 1]
            line.append(row + base)
            base = base + row[:, LANES - 1 :]
        places.append(jnp.concatenate(line, 1).astype(jnp.int32) - 1)
    place = jnp.where(leaving[0], places[0], jnp.where(leaving[1], MOVE + places[1], -1))
    chosen = one_hot(place, 2 * MOVE)
    copies[1].wait()
    copies[2].wait()
    payload_ref[:BLOCK] = rhs[...]
    payload_ref[BLOCK : BLOCK + 1] = cond[...]
    payload_ref[BLOCK + 1 : BLOCK + 2] = as_f32(slot + 1)
    payload_ref[BLOCK + 2 : ROWS] = jnp.zeros((ROWS - BLOCK - 2, cells), jnp.float32)
    out = dot_rows(chosen, jnp.concatenate(parts_of(payload_ref[...], 3), 0))
    packed = out[:, :ROWS] + (out[:, ROWS : 2 * ROWS] + out[:, 2 * ROWS :])
    left_ref[...] = packed[:MOVE]
    right_ref[...] = packed[MOVE:]


def stay_kernel(payload_ref, stay_ref, send_ref, neighbour_ref, placed_ref, send_hot_ref, ghost_hot_ref):
    cells = stay_ref.shape[1]
    ghosts = send_ref.shape[1]
    out = dot_rows(jnp.concatenate(parts_of(payload_ref[...], 3), 0), one_hot(stay_ref[...], cells))
    placed_ref[...] = out[:ROWS] + (out[ROWS : 2 * ROWS] + out[2 * ROWS :])
    for side in range(2):
        send_hot_ref[side] = one_hot(send_ref[side : side + 1], cells)
        ghost_hot_ref[side] = one_hot(neighbour_ref[side : side + 1], ghosts, cells + side * ghosts)


def fill_faces(data_ref, out, kappa, count):
    row = lax.broadcasted_iota(jnp.int32, (HALF, 1), 0)
    for face in range(count):
        start = face * SLAB
        data_ref[start : start + HALF] = jnp.where(row == FACE, kappa, out[start : start + HALF])
        data_ref[start + HALF : start + SLAB] = kappa * out[start + HALF : start + SLAB]


def boundary(field, kappa, trace_ref, send_hot_ref, pair_ref, left_ref, right_ref):
    fill_faces(pair_ref, times3(trace_ref[...], field), kappa, 2)
    left_ref[...] = pick(pair_ref[:SLAB], send_hot_ref[0], 2)
    right_ref[...] = pick(pair_ref[SLAB:], send_hot_ref[1], 2)


def arrive_kernel(placed_ref, from_left_ref, from_right_ref, trace_ref, send_hot_ref,
                  field_ref, kappa_ref, pair_ref, left_ref, right_ref):
    cells = placed_ref.shape[1]
    records = jnp.concatenate([from_left_ref[...], from_right_ref[...]], 0)
    slot = records[:, BLOCK + 1 : BLOCK + 2].astype(jnp.int32) - 1
    ids = lax.broadcasted_iota(jnp.int32, (2 * MOVE, cells), 1)
    chosen = as_bf16(jnp.where(ids == slot, 1.0, 0.0))
    merged = placed_ref[...] + pick(records.T, chosen, 3)
    kappa = merged[BLOCK : BLOCK + 1]
    row = lax.broadcasted_iota(jnp.int32, (ROWS, 1), 0)
    field = jnp.where(row < BLOCK, merged, 0.0)
    field_ref[...] = field
    kappa_ref[...] = kappa
    boundary(field, kappa, trace_ref, send_hot_ref, pair_ref, left_ref, right_ref)


def face_jumps(face, near, own, kappa, neighbour_ref, code_ref, flips):
    code = code_ref[face : face + 1]
    first = as_f32(jnp.bitwise_and(code, 1))
    second = as_f32(jnp.right_shift(code, 1))
    sign = (1.0 - 2.0 * first * flips[:, 0:1]) * (1.0 - 2.0 * second * flips[:, 1:2])
    outside = jnp.where(neighbour_ref[face : face + 1] < 0, 2.0, 1.0)
    jump = outside * own - sign * near
    strength = PENALTY * jnp.maximum(kappa, near[FACE : FACE + 1])
    return jump[:HALF], jump[HALF:], strength


def face_terms(jumps, kappa):
    values, fluxes, strength = jumps
    return jnp.concatenate([strength * values - 0.5 * fluxes, kappa * values], 0)


def one_sided(jumps, own):
    values, fluxes, strength = jumps
    return own[:HALF] * (strength * values - 0.5 * fluxes) - 0.5 * own[HALF:] * values


def both_sided(jumps):
    values, fluxes, strength = jumps
    return values * (strength * values - fluxes)


def local_terms(field_ref, kappa_ref, pair_ref, neighbour_ref, code_ref, trace_ref, back_ref, weight_ref,
                flip_ref, part_ref, near_ref, rest, energy):
    cells = field_ref.shape[1]
    kappa = kappa_ref[...]
    flips = flip_ref[...]
    field = field_ref[...]
    inner = FACES - 2
    out = times3(trace_ref[...], field)
    fill_faces(rest, out, kappa, inner)
    terms = []
    total = jnp.zeros((HALF, cells), jnp.float32)
    for face in range(FACES):
        source, base = (pair_ref, 0) if face < 2 else (rest, 2)
        other = ((face ^ 1) - base) * SLAB
        near = pick(source[other : other + SLAB], one_hot(neighbour_ref[face : face + 1], cells), 2)
        own = source[(face - base) * SLAB : (face - base + 1) * SLAB]
        if face < 2:
            near_ref[face * SLAB : (face + 1) * SLAB] = near
            if face == 0 or not energy:
                continue
        jumps = face_jumps(face, near, own, kappa, neighbour_ref, code_ref, flips)
        if energy:
            share = one_sided(jumps, own)
            if face == 1:
                total = total + jnp.where(neighbour_ref[1:2] < cells, share, 0.0)
                continue
            total = total + share
        terms.append(face_terms(jumps, kappa))
    volume = weight_ref[...] * field + kappa * out[inner * SLAB :]
    part_ref[...] = volume + times3(back_ref[...], jnp.concatenate(terms, 0))
    return volume, flips[:HALF, 2:3] * total


def first_kernel(field_ref, kappa_ref, pair_ref, neighbour_ref, code_ref, trace_ref, back_ref, weight_ref,
                 flip_ref, part_ref, near_ref, rest):
    local_terms(field_ref, kappa_ref, pair_ref, neighbour_ref, code_ref, trace_ref, back_ref, weight_ref,
                flip_ref, part_ref, near_ref, rest, False)


def whole_sum(value):
    return jnp.sum(jnp.sum(value, axis=0, keepdims=True), axis=1, keepdims=True)


def second_kernel(image_ref, kappa_ref, pair_ref, neighbour_ref, code_ref, trace_ref, back_ref, weight_ref,
                  flip_ref, field_ref, part_ref, near_ref, sums_ref, rest):
    volume, faces = local_terms(image_ref, kappa_ref, pair_ref, neighbour_ref, code_ref, trace_ref, back_ref,
                                weight_ref, flip_ref, part_ref, near_ref, rest, True)
    field, image = field_ref[...], image_ref[...]
    totals = (whole_sum(field * field), whole_sum(field * image), whole_sum(image * image),
              whole_sum(image * volume) + whole_sum(faces))
    lane = lax.broadcasted_iota(jnp.int32, (1, LANES), 1)
    sums = jnp.zeros((1, LANES), jnp.float32)
    for place, total in enumerate(totals):
        sums = jnp.where(lane == place, total, sums)
    sums_ref[...] = sums


def ghost_jumps(face, ghost_ref, near_ref, pair_ref, kappa, neighbour_ref, code_ref, flips, ghost_hot_ref):
    rows = slice(face * SLAB, (face + 1) * SLAB)
    near = near_ref[rows] + pick(ghost_ref[...], ghost_hot_ref[face], 2)
    return face_jumps(face, near, pair_ref[rows], kappa, neighbour_ref, code_ref, flips)


def middle_kernel(part_ref, near_ref, pair_ref, kappa_ref, from_left_ref, from_right_ref, neighbour_ref,
                  code_ref, back_ref, flip_ref, trace_ref, send_hot_ref, ghost_hot_ref,
                  image_ref, next_ref, left_ref, right_ref):
    kappa = kappa_ref[...]
    terms = [
        face_terms(ghost_jumps(face, ref, near_ref, pair_ref, kappa, neighbour_ref, code_ref, flip_ref[...],
                               ghost_hot_ref), kappa)
        for face, ref in ((0, from_left_ref), (1, from_right_ref))
    ]
    image = part_ref[...] + times3(back_ref[...], jnp.concatenate(terms, 0))
    image_ref[...] = image
    boundary(image, kappa, trace_ref, send_hot_ref, next_ref, left_ref, right_ref)


def energy_kernel(near_ref, pair_ref, kappa_ref, from_left_ref, neighbour_ref, code_ref, flip_ref,
                  ghost_hot_ref, partial_ref, sums_ref, term_ref):
    cells = near_ref.shape[1]
    kappa = kappa_ref[...]
    flips = flip_ref[...]
    jumps = ghost_jumps(0, from_left_ref, near_ref, pair_ref, kappa, neighbour_ref, code_ref, flips,
                        ghost_hot_ref)
    term_ref[...] = face_terms(jumps, kappa)
    shared = jnp.where(neighbour_ref[0:1] < cells, one_sided(jumps, pair_ref[:SLAB]), both_sided(jumps))
    total = whole_sum(flips[:HALF, 2:3] * shared)
    lane = lax.broadcasted_iota(jnp.int32, (1, LANES), 1)
    sums = partial_ref[...] + jnp.where(lane == 3, total, 0.0)
    sums_ref[...] = jnp.broadcast_to(sums, sums_ref.shape)


def update_kernel(sums_ref, field_ref, image_ref, part_ref, term_ref, near_ref, pair_ref, kappa_ref,
                  from_right_ref, neighbour_ref, code_ref, back_ref, flip_ref, ghost_hot_ref,
                  solution_ref, residual_ref):
    kappa = kappa_ref[...]
    jumps = ghost_jumps(1, from_right_ref, near_ref, pair_ref, kappa, neighbour_ref, code_ref, flip_ref[...],
                        ghost_hot_ref)
    terms = jnp.concatenate([term_ref[...], face_terms(jumps, kappa)], 0)
    twice = (part_ref[...] + times3(back_ref[...], terms))[:BLOCK]
    sums = jnp.sum(sums_ref[...], axis=0, keepdims=True)
    bb, bw, ww, wt = (sums[:, place : place + 1] for place in range(4))
    alpha = bb / bw
    rr = bb - 2.0 * alpha * bw + alpha * alpha * ww
    beta = rr / bb
    more = 1.0 + beta
    inner = more * more * bw - 2.0 * alpha * more * ww + alpha * alpha * wt
    step = rr / inner
    field, image = field_ref[:BLOCK], image_ref[:BLOCK]
    solution_ref[...] = (alpha + step * more) * field - (step * alpha) * image
    residual_ref[...] = (field - alpha * image) - step * (more * image - alpha * twice)


def to_next(value):
    count = lax.axis_size(AXES)
    return lax.ppermute(value, AXES, [(i, (i + 1) % count) for i in range(count)])


def to_previous(value):
    count = lax.axis_size(AXES)
    return lax.ppermute(value, AXES, [((i + 1) % count, i) for i in range(count)])


def body(right_side, conductivity, destination, neighbour, orientation, send_list):
    constants = (jnp.asarray(table) for table in operator_constants())
    trace_pair, trace_rest, back_ghost, back_local, weight_rows, flips = constants
    cells = destination.shape[0]
    ghosts = send_list.shape[1]
    whole, slab, row = f32(ROWS, cells), f32(SLAB, ghosts), f32(1, cells)
    pair = f32(2 * SLAB, cells)
    big = 2 * ROWS * cells
    left, right, payload, stay = call(
        pack_kernel, [f32(MOVE, ROWS)] * 2 + [whole, jax.ShapeDtypeStruct((1, cells), jnp.int32)],
        [right_side, conductivity[None], destination[None]], big * LANES * 3,
        [pltpu.VMEM((BLOCK, cells), jnp.float32), pltpu.VMEM((1, cells), jnp.float32),
         pltpu.VMEM((1, cells), jnp.int32), pltpu.SemaphoreType.DMA((3,))],
        "pack", far=3)
    from_right = to_previous(left)
    from_left = to_next(right)
    placed, send_hot, ghost_hot = call(
        stay_kernel,
        [whole, jax.ShapeDtypeStruct((2, cells, ghosts), jnp.bfloat16),
         jax.ShapeDtypeStruct((2, ghosts, cells), jnp.bfloat16)],
        [payload, stay, send_list, neighbour], big * cells * 3, (), "stay")
    field, kappa, faces, left, right = call(
        arrive_kernel, [whole, row, pair, slab, slab],
        [placed, from_left, from_right, trace_pair, send_hot], big * 2 * SLAB * 3, (), "arrive")
    from_right = to_previous(left)
    from_left = to_next(right)
    rest = [pltpu.VMEM(((FACES - 2) * SLAB, cells), jnp.float32)]
    shared = [neighbour, orientation, trace_rest, back_local, weight_rows, flips]
    part, near = call(first_kernel, [whole, pair], [field, kappa, faces] + shared,
                      big * cells * FACES * 2, rest, "first")
    image, faces, left, right = call(
        middle_kernel, [whole, pair, slab, slab],
        [part, near, faces, kappa, from_left, from_right, neighbour, orientation, back_ghost, flips,
         trace_pair, send_hot, ghost_hot], big * 2 * SLAB * 3, (), "middle")
    from_left = to_next(right)
    from_right = to_previous(left)
    part, near, partial = call(second_kernel, [whole, pair, f32(1, LANES)],
                               [image, kappa, faces] + shared + [field], big * cells * FACES * 2, rest, "second")
    sums, term = call(
        energy_kernel, [f32(lax.axis_size(AXES), LANES), f32(SLAB, cells)],
        [near, faces, kappa, from_left, neighbour, orientation, flips, ghost_hot, partial],
        big * SLAB * 2, (), "energy")
    sums = lax.all_to_all(sums, AXES, 0, 0, tiled=True)
    return tuple(call(
        update_kernel, [f32(BLOCK, cells)] * 2,
        [sums, field, image, part, term, near, faces, kappa, from_right, neighbour, orientation, back_ghost,
         flips, ghost_hot], big * 2 * SLAB * 3, (), "update"))


def solution(mesh):
    in_specs = (
        P(None, AXES),
        P(AXES),
        P(AXES),
        P(None, AXES),
        P(None, AXES),
        P(None, AXES),
    )
    out_specs = (P(None, AXES), P(None, AXES))
    return jax.shard_map(body, mesh=mesh, in_specs=in_specs, out_specs=out_specs, check_vma=False)
```

```python
import functools

import jax
import jax.numpy as jnp
import numpy as np
from jax import lax
from jax.experimental import pallas as pl
from jax.experimental.pallas import tpu as pltpu
from jax.sharding import PartitionSpec as P


NODES = 5
FACE = NODES * NODES
BLOCK = NODES**3
MOVE = 64
LANES = 128
ROWS = 128
HALF = 32
SLAB = 2 * HALF
FACES = 6
PENALTY = 80.0
AXES = ("curve", "group")
VMEM_LIMIT = 24 * 1024 * 1024

GAUSS_POINTS = (-0.906179845938664, -0.5384693101056831, 0.0, 0.5384693101056831, 0.906179845938664)
GAUSS_WEIGHTS = (
    0.2369268850561891,
    0.4786286704993665,
    0.5688888888888889,
    0.4786286704993665,
    0.2369268850561891,
)


def lagrange_value(points, position, location):
    value = 1.0
    for other in range(len(points)):
        if other != position:
            value = value * (location - points[other]) / (points[position] - points[other])
    return value


def lagrange_slope(points, position, location):
    total = 0.0
    for skipped in range(len(points)):
        if skipped == position:
            continue
        addend = 1.0 / (points[position] - points[skipped])
        for other in range(len(points)):
            if other != position and other != skipped:
                addend = addend * (location - points[other]) / (points[position] - points[other])
        total = total + addend
    return total


def basis_tables():
    points = [0.5 * (value + 1.0) for value in GAUSS_POINTS]
    weights = [0.5 * value for value in GAUSS_WEIGHTS]
    count = len(points)
    slopes = [[lagrange_slope(points, p, points[q]) for p in range(count)] for q in range(count)]
    start_value = [lagrange_value(points, p, 0.0) for p in range(count)]
    end_value = [lagrange_value(points, p, 1.0) for p in range(count)]
    start_slope = [-lagrange_slope(points, p, 0.0) for p in range(count)]
    end_slope = [lagrange_slope(points, p, 1.0) for p in range(count)]
    listed = (weights, slopes, start_value, end_value, start_slope, end_slope)
    return [np.asarray(np.asarray(table, np.float32), np.float64) for table in listed]


def along_axis(matrix, axis_id):
    factors = [np.eye(NODES)] * 3
    factors[axis_id] = matrix
    return np.kron(factors[0], np.kron(factors[1], factors[2]))


def parity_basis():
    root = np.sqrt(0.5)
    line = np.zeros((NODES, NODES))
    line[0, 0] = line[0, 4] = line[1, 1] = line[1, 3] = root
    line[2, 2] = 1.0
    line[3, 0], line[3, 4] = root, -root
    line[4, 1], line[4, 3] = root, -root
    odd = np.array([0, 0, 0, 1, 1])
    return np.kron(line, line), np.repeat(odd, NODES), np.tile(odd, NODES)


def split_two(matrix):
    high = matrix.astype(np.float32).astype(jnp.bfloat16)
    low = (matrix - high.astype(np.float64)).astype(np.float32).astype(jnp.bfloat16)
    return high, low


@functools.cache
def operator_constants():
    weights, slopes, *ends = basis_tables()
    cell_weight = np.kron(weights, np.kron(weights, weights))
    face_weight = np.kron(weights, weights)
    parity, odd_first, odd_second = parity_basis()
    stiff = np.zeros((BLOCK, BLOCK))
    for axis_id in range(3):
        grad = along_axis(slopes, axis_id)
        stiff += grad.T @ (cell_weight[:, None] * grad)
    trace = np.zeros((FACES * SLAB + ROWS, ROWS))
    back = np.zeros((ROWS, FACES * SLAB))
    for face in range(FACES):
        tangent = along_axis(ends[face % 2][None, :], face // 2)
        normal = along_axis(ends[2 + face % 2][None, :], face // 2)
        start = face * SLAB
        trace[start : start + FACE, :BLOCK] = parity @ tangent
        trace[start + HALF : start + HALF + FACE, :BLOCK] = parity @ normal
        spread = (face_weight[:, None] * parity.T)
        back[:BLOCK, start : start + FACE] = tangent.T @ spread
        back[:BLOCK, start + HALF : start + HALF + FACE] = -0.5 * normal.T @ spread
    trace[FACES * SLAB : FACES * SLAB + BLOCK, :BLOCK] = stiff
    high, low = split_two(trace)
    trace3 = np.concatenate([high, high, low], 1)
    trace_pair, trace_rest = trace3[: 2 * SLAB], trace3[2 * SLAB :]
    backs = []
    for first, last in ((0, 2), (2, FACES)):
        high, low = split_two(back[:, first * SLAB : last * SLAB])
        backs.append(np.concatenate([high, high, low], 1))
    weight_rows = np.zeros((ROWS, 1), np.float32)
    weight_rows[:BLOCK, 0] = cell_weight
    flips = np.zeros((SLAB, LANES), np.float32)
    for start in (0, HALF):
        flips[start : start + FACE, 0] = odd_first
        flips[start : start + FACE, 1] = odd_second
        flips[start : start + FACE, 2] = np.diag(parity @ (face_weight[:, None] * parity.T))
    return trace_pair, trace_rest, backs[0], backs[1], weight_rows, flips


def as_bf16(value):
    return value.astype(jnp.bfloat16)


def as_f32(value):
    return value.astype(jnp.float32)


def parts_of(value, count):
    pieces = []
    for step in range(count):
        piece = as_bf16(value)
        pieces.append(piece)
        if step + 1 < count:
            value = value - as_f32(piece)
    return pieces


def dot(left, right):
    return lax.dot_general(left, right, (((1,), (0,)), ((), ())), preferred_element_type=jnp.float32)


def dot_rows(left, right):
    return lax.dot_general(left, right, (((1,), (1,)), ((), ())), preferred_element_type=jnp.float32)


def times3(table3, value):
    high, low = parts_of(value, 2)
    return dot(table3, jnp.concatenate([high, low, high], 0))


def pick(value, chosen, count):
    rows = value.shape[0]
    out = dot(jnp.concatenate(parts_of(value, count), 0), chosen)
    total = out[(count - 1) * rows :]
    for step in reversed(range(count - 1)):
        total = total + out[step * rows : (step + 1) * rows]
    return total


def one_hot(index_row, rows, offset=0):
    ids = lax.broadcasted_iota(jnp.int32, (rows, index_row.shape[1]), 0)
    return as_bf16(jnp.where(ids == index_row - offset, 1.0, 0.0))


def call(kernel, outs, args, flops, scratch=(), far=0, out=pltpu.VMEM):
    moved = sum(a.size * a.dtype.itemsize for a in args) + sum(o.size * o.dtype.itemsize for o in outs)
    spaces = [pltpu.MemorySpace.HBM] * far + [pltpu.VMEM] * (len(args) - far)
    args = [pltpu.with_memory_space_constraint(a, pltpu.MemorySpace.HBM) if i < far else a
            for i, a in enumerate(args)]
    return pl.pallas_call(
        kernel,
        out_shape=list(outs),
        in_specs=[pl.BlockSpec(memory_space=space) for space in spaces],
        out_specs=[pl.BlockSpec(memory_space=out) for _ in outs],
        scratch_shapes=list(scratch),
        compiler_params=pltpu.CompilerParams(vmem_limit_bytes=VMEM_LIMIT),
        cost_estimate=pl.CostEstimate(flops=flops, bytes_accessed=moved, transcendentals=0),
    )(*args)


def f32(*shape):
    return jax.ShapeDtypeStruct(shape, jnp.float32)


def my_rank():
    return lax.axis_index("curve") * lax.axis_size("group") + lax.axis_index("group")


def pack_kernel(rhs_hbm, cond_hbm, dest_hbm, send_hbm, trace_hbm, nbr_hbm, near_up_ref, near_down_ref, far_up_ref,
                far_down_ref, packed_ref, payload_ref, stay_ref, send, nbr, trace, rhs, cond, dest_row, sems):
    cells = dest_row.shape[1]
    tiles = cells // LANES
    copies = [
        pltpu.make_async_copy(source, target, sems.at[place])
        for place, (source, target) in enumerate(
            ((dest_hbm, dest_row), (send_hbm, send), (cond_hbm, cond), (rhs_hbm, rhs), (trace_hbm, trace),
             (nbr_hbm, nbr))
        )
    ]
    for copy in copies:
        copy.start()
    copies[0].wait()
    copies[1].wait()
    dest = dest_row[...]
    owner = lax.div(dest, cells)
    target, slot = owner - my_rank(), dest - owner * cells
    stay = jnp.where(target == 0, slot, -1)
    stay_ref[...] = stay
    leaving = [target == -1, target == 1]
    marks = [as_f32(mask) for mask in leaving]
    stacked = jnp.concatenate(
        [mark[:, t * LANES : (t + 1) * LANES] for mark in marks for t in range(tiles)], 0
    )
    first = lax.broadcasted_iota(jnp.int32, (LANES, LANES), 0)
    second = lax.broadcasted_iota(jnp.int32, (LANES, LANES), 1)
    counts = dot(as_bf16(stacked), as_bf16(jnp.where(first <= second, 1.0, 0.0)))
    places = []
    for side in range(2):
        base = jnp.zeros((1, 1), jnp.float32)
        line = []
        for t in range(tiles):
            row = counts[side * tiles + t : side * tiles + t + 1]
            line.append(row + base)
            base = base + row[:, LANES - 1 :]
        places.append(jnp.concatenate(line, 1).astype(jnp.int32) - 1)
    place = jnp.where(leaving[0], places[0], jnp.where(leaving[1], MOVE + places[1], -1))
    chosen = one_hot(place, 2 * MOVE)
    lists = as_f32(send[...])
    columns = jnp.concatenate([lists, jnp.zeros((6, lists.shape[1]), jnp.float32)], 0).T
    stay_row = as_f32(stay)
    kept = [as_bf16(jnp.where(columns[:, side : side + 1] == stay_row, 1.0, 0.0)) for side in range(2)]
    for copy in copies[2:]:
        copy.wait()
    payload_ref[:BLOCK] = rhs[...]
    payload_ref[BLOCK : BLOCK + 1] = cond[...]
    payload_ref[BLOCK + 1 : BLOCK + 2] = as_f32(slot + 1)
    payload_ref[BLOCK + 2 : ROWS] = jnp.zeros((ROWS - BLOCK - 2, cells), jnp.float32)
    payload = payload_ref[...]
    out = dot_rows(chosen, jnp.concatenate(parts_of(payload, 2), 0))
    packed = out[:, :ROWS] + out[:, ROWS:]
    packed_ref[...] = packed
    traces = face_rows(times3(trace[...], payload), cond[...], 2)
    sides = []
    for side in range(2):
        out = dot_rows(jnp.concatenate(parts_of(traces[side], 2), 0), kept[side])
        ghosts = out[:SLAB] + out[SLAB:]
        row = lax.broadcasted_iota(jnp.int32, (SLAB, 1), 0)
        ghosts = jnp.where(row == FACE + 1, lists[side : side + 1] + 1.0, ghosts)
        moving = packed[side * MOVE : (side + 1) * MOVE]
        half = MOVE // 2
        sides.append(jnp.concatenate([ghosts, jnp.concatenate([moving[:half], moving[half:]], 1)], 0))
    near_up_ref[...] = sides[1]
    near_down_ref[...] = sides[0]
    far_up_ref[...] = packed[MOVE:]
    far_down_ref[...] = packed[:MOVE]


def stay_kernel(count, *refs):
    far, (payload_ref, stay_ref, send_ref, neighbour_ref) = refs[:count], refs[count : count + 4]
    placed_ref, send_hot_ref, ghost_hot_ref, hot_ref = refs[count + 4 : count + 8]
    close, sems = refs[count + 8 : -1], refs[-1]
    copies = [pltpu.make_async_copy(far[k], close[k], sems.at[k]) for k in range(count)]
    for copy in copies:
        copy.start()
    cells = stay_ref.shape[1]
    ghosts = send_ref.shape[1]
    out = dot_rows(jnp.concatenate(parts_of(payload_ref[...], 3), 0), one_hot(stay_ref[...], cells))
    placed_ref[...] = out[:ROWS] + (out[ROWS : 2 * ROWS] + out[2 * ROWS :])
    for side in range(2):
        send_hot_ref[side] = one_hot(send_ref[side : side + 1], cells)
        ghost_hot_ref[side] = one_hot(neighbour_ref[side : side + 1], ghosts, cells + side * ghosts)
    for face in range(FACES):
        hot_ref[face] = one_hot(neighbour_ref[face : face + 1], cells)
    for copy in copies:
        copy.wait()


def face_rows(out, kappa, count):
    row = lax.broadcasted_iota(jnp.int32, (HALF, 1), 0)
    slabs = []
    for face in range(count):
        start = face * SLAB
        values = jnp.where(row == FACE, kappa, out[start : start + HALF])
        slabs.append(jnp.concatenate([values, kappa * out[start + HALF : start + SLAB]], 0))
    return slabs


def moved_ghosts(records, lists, trace_ref):
    columns = records.T
    slabs = face_rows(times3(trace_ref[...], columns), columns[BLOCK : BLOCK + 1], 2)
    slots = records[:, BLOCK + 1 : BLOCK + 2]
    side_of = lax.broadcasted_iota(jnp.int32, (2 * MOVE, 1), 0) // MOVE
    found = []
    for side in range(2):
        wanted = jnp.where(side_of == side, slots, -1.0)
        found.append(pick(slabs[1 - side], as_bf16(jnp.where(wanted == lists[side], 1.0, 0.0)), 2))
    return found


def face_jumps(face, near, own, kappa, neighbour_ref, code_ref, flips):
    code = code_ref[face : face + 1]
    first = 1.0 - 2.0 * as_f32(jnp.bitwise_and(code, 1))
    second = 1.0 - 2.0 * as_f32(jnp.right_shift(code, 1))
    sign = jnp.where(flips[:HALF, 0:1] > 0.0, first, 1.0) * jnp.where(flips[:HALF, 1:2] > 0.0, second, 1.0)
    outside = jnp.where(neighbour_ref[face : face + 1] < 0, 2.0, 1.0)
    strength = PENALTY * jnp.maximum(kappa, near[FACE : FACE + 1])
    values = outside * own[:HALF] - sign * near[:HALF]
    return values, outside * own[HALF:] - sign * near[HALF:], strength


def face_terms(jumps, kappa):
    values, fluxes, strength = jumps
    return jnp.concatenate([strength * values - 0.5 * fluxes, kappa * values], 0)


def one_sided(jumps, own):
    values, fluxes, strength = jumps
    return own[:HALF] * (strength * values - 0.5 * fluxes) - 0.5 * own[HALF:] * values


def both_sided(jumps):
    values, fluxes, strength = jumps
    return values * (strength * values - fluxes)


def first_kernel(placed_ref, near_up_ref, near_down_ref, far_up_ref, far_down_ref, packed_ref, pair_trace_ref,
                 neighbour_ref, code_ref, trace_ref, back_ref, back_ghost_ref, weight_ref, flip_ref, send_hot_ref,
                 ghost_hot_ref, hot_ref, field_ref, kappa_ref, image_ref, pair_ref, right_ref):
    cells = placed_ref.shape[1]
    buffers = (near_up_ref[...], near_down_ref[...])
    records = jnp.concatenate(
        [piece for buffer in buffers for piece in (buffer[SLAB:, :LANES], buffer[SLAB:, LANES:])], 0
    )
    slot = records[:, BLOCK + 1 : BLOCK + 2].astype(jnp.int32) - 1
    ids = lax.broadcasted_iota(jnp.int32, (2 * MOVE, cells), 1)
    merged = placed_ref[...] + pick(records.T, as_bf16(jnp.where(ids == slot, 1.0, 0.0)), 2)
    kappa = merged[BLOCK : BLOCK + 1]
    row = lax.broadcasted_iota(jnp.int32, (ROWS, 1), 0)
    field = jnp.where(row < BLOCK, merged, 0.0)
    field_ref[...] = field
    kappa_ref[...] = kappa
    pair = face_rows(times3(pair_trace_ref[...], field), kappa, 2)
    out = times3(trace_ref[...], field)
    slabs = pair + face_rows(out, kappa, FACES - 2)
    lists = [buffer[FACE + 1 : FACE + 2] for buffer in buffers]
    far = jnp.concatenate([far_up_ref[...], far_down_ref[...]], 0)
    moved = [moved_ghosts(some, lists, pair_trace_ref) for some in (packed_ref[...], far)]
    flips = flip_ref[...]
    terms = []
    for face in range(FACES):
        near = pick(slabs[face ^ 1], hot_ref[face], 2)
        if face < 2:
            ghosts = buffers[face][:SLAB] + (moved[0][face] + moved[1][face])
            near = near + pick(ghosts, ghost_hot_ref[face], 2)
        jumps = face_jumps(face, near, slabs[face], kappa, neighbour_ref, code_ref, flips)
        terms.append(face_terms(jumps, kappa))
    volume = weight_ref[...] * field + kappa * out[(FACES - 2) * SLAB :]
    image = (volume + times3(back_ref[...], jnp.concatenate(terms[2:], 0))
             + times3(back_ghost_ref[...], jnp.concatenate(terms[:2], 0)))
    image_ref[...] = image
    pair_ref[:SLAB], pair_ref[SLAB:] = face_rows(times3(pair_trace_ref[...], image), kappa, 2)
    right_ref[...] = pick(pair_ref[SLAB:], send_hot_ref[1], 2)


def whole_sum(value):
    return jnp.sum(jnp.sum(value, axis=0, keepdims=True), axis=1, keepdims=True)


def second_kernel(image_ref, kappa_ref, pair_ref, neighbour_ref, code_ref, trace_ref, back_ref, weight_ref,
                  flip_ref, hot_ref, send_hot_ref, field_ref, part_ref, near_ref, sums_ref, left_ref):
    left_ref[...] = pick(pair_ref[:SLAB], send_hot_ref[0], 2)
    cells = image_ref.shape[1]
    kappa = kappa_ref[...]
    flips = flip_ref[...]
    field, image = field_ref[...], image_ref[...]
    out = times3(trace_ref[...], image)
    slabs = face_rows(out, kappa, FACES - 2)
    total = jnp.zeros((HALF, cells), jnp.float32)
    terms = []
    for face in range(FACES):
        slab = pair_ref[(1 - face) * SLAB : (2 - face) * SLAB] if face < 2 else slabs[(face ^ 1) - 2]
        near = pick(slab, hot_ref[face], 2)
        if face < 2:
            near_ref[face * SLAB : (face + 1) * SLAB] = near
        if face == 0:
            continue
        own = pair_ref[SLAB:] if face == 1 else slabs[face - 2]
        jumps = face_jumps(face, near, own, kappa, neighbour_ref, code_ref, flips)
        share = one_sided(jumps, own)
        if face == 1:
            total = total + jnp.where(neighbour_ref[1:2] < cells, share, 0.0)
        else:
            total = total + share
            terms.append(face_terms(jumps, kappa))
    volume = weight_ref[...] * image + kappa * out[(FACES - 2) * SLAB :]
    part_ref[...] = volume + times3(back_ref[...], jnp.concatenate(terms, 0))
    totals = (whole_sum(field * field), whole_sum(field * image), whole_sum(image * image),
              whole_sum(image * volume) + whole_sum(flips[:HALF, 2:3] * total))
    lane = lax.broadcasted_iota(jnp.int32, (1, LANES), 1)
    sums = jnp.zeros((1, LANES), jnp.float32)
    for place, value in enumerate(totals):
        sums = jnp.where(lane == place, value, sums)
    sums_ref[...] = sums


def ghost_jumps(face, ghosts, near_ref, pair_ref, kappa, neighbour_ref, code_ref, flips, ghost_hot_ref):
    rows = slice(face * SLAB, (face + 1) * SLAB)
    near = near_ref[rows] + pick(ghosts, ghost_hot_ref[face], 2)
    return face_jumps(face, near, pair_ref[rows], kappa, neighbour_ref, code_ref, flips)


def energy_kernel(near_ref, pair_ref, kappa_ref, from_left_ref, neighbour_ref, code_ref, flip_ref,
                  ghost_hot_ref, partial_ref, sums_ref, term_ref):
    cells = near_ref.shape[1]
    kappa = kappa_ref[...]
    flips = flip_ref[...]
    jumps = ghost_jumps(0, from_left_ref[...], near_ref, pair_ref, kappa, neighbour_ref, code_ref, flips,
                        ghost_hot_ref)
    term_ref[...] = face_terms(jumps, kappa)
    shared = jnp.where(neighbour_ref[0:1] < cells, one_sided(jumps, pair_ref[:SLAB]), both_sided(jumps))
    total = whole_sum(flips[:HALF, 2:3] * shared)
    lane = lax.broadcasted_iota(jnp.int32, (1, LANES), 1)
    sums = partial_ref[...] + jnp.where(lane == 3, total, 0.0)
    sums_ref[...] = jnp.broadcast_to(sums, sums_ref.shape)


def update_kernel(sums_ref, field_ref, image_ref, part_ref, edge_ref, near_ref, pair_ref, kappa_ref,
                  from_right_ref, neighbour_ref, code_ref, back_ref, flip_ref, ghost_hot_ref,
                  solution_hbm, residual_hbm, solution, residual, sems):
    sums = sums_ref[...]
    bb, bw, ww, wt = (sums[:, place : place + 1] for place in range(4))
    alpha = bb / bw
    rr = bb - 2.0 * alpha * bw + alpha * alpha * ww
    beta = rr / bb
    more = 1.0 + beta
    inner = more * more * bw - 2.0 * alpha * more * ww + alpha * alpha * wt
    step = rr / inner
    field, image = field_ref[:BLOCK], image_ref[:BLOCK]
    solution[...] = (alpha + step * more) * field - (step * alpha) * image
    first = pltpu.make_async_copy(solution, solution_hbm, sems.at[0])
    first.start()
    kappa = kappa_ref[...]
    jumps = ghost_jumps(1, from_right_ref[...], near_ref, pair_ref, kappa, neighbour_ref, code_ref,
                        flip_ref[...], ghost_hot_ref)
    edges = jnp.concatenate([edge_ref[...], face_terms(jumps, kappa)], 0)
    twice = part_ref[...] + times3(back_ref[...], edges)
    residual[...] = field - (alpha + step * more) * image + (step * alpha) * twice[:BLOCK]
    second = pltpu.make_async_copy(residual, residual_hbm, sems.at[1])
    second.start()
    first.wait()
    second.wait()


def shift(value, distance):
    count = lax.axis_size(AXES)
    return lax.ppermute(value, AXES, [(i, (i + distance) % count) for i in range(count)])


def bf16(*shape):
    return jax.ShapeDtypeStruct(shape, jnp.bfloat16)


def i32(*shape):
    return jax.ShapeDtypeStruct(shape, jnp.int32)


def body(right_side, conductivity, destination, neighbour, orientation, send_list):
    constants = (jnp.asarray(table) for table in operator_constants())
    trace_pair, trace_rest, back_ghost, back_local, weight_rows, flips = constants
    devices = lax.axis_size(AXES)
    cells = destination.shape[0]
    ghosts = send_list.shape[1]
    whole, slab, row = f32(ROWS, cells), f32(SLAB, ghosts), f32(1, cells)
    pair = f32(2 * SLAB, cells)
    big = 2 * ROWS * cells
    near_up, near_down, far_up, far_down, packed, payload, stay, send, nbr, trace_pair = call(
        pack_kernel,
        [f32(SLAB + MOVE // 2, ghosts)] * 2 + [f32(MOVE, ROWS)] * 2
        + [f32(2 * MOVE, ROWS), whole, i32(1, cells), i32(2, ghosts), i32(FACES, cells), bf16(*trace_pair.shape)],
        [right_side, conductivity[None], destination[None], send_list, trace_pair, neighbour], big * LANES * 6,
        [pltpu.VMEM((BLOCK, cells), jnp.float32), pltpu.VMEM((1, cells), jnp.float32),
         pltpu.VMEM((1, cells), jnp.int32), pltpu.SemaphoreType.DMA((6,))],
        far=6)
    near_up = shift(near_up, 1)
    far_up = shift(far_up, 2)
    far_down = shift(far_down, -2)
    near_down = shift(near_down, -1)
    later = [orientation, trace_rest, back_local, back_ghost, weight_rows, flips]
    placed, send_hot, ghost_hot, hot, *later = call(
        functools.partial(stay_kernel, len(later)),
        [whole, bf16(2, cells, ghosts), bf16(2, ghosts, cells), bf16(FACES, cells, cells)]
        + [jax.ShapeDtypeStruct(a.shape, a.dtype) for a in later],
        later + [payload, stay, send, nbr], big * cells * 3, [pltpu.SemaphoreType.DMA((len(later),))],
        far=len(later))
    orientation, trace_rest, back_local, back_ghost, weight_rows, flips = later
    field, kappa, image, faces, right = call(
        first_kernel, [whole, row, whole, pair, slab],
        [placed, near_up, near_down, far_up, far_down, packed, trace_pair, nbr, orientation, trace_rest,
         back_local, back_ghost, weight_rows, flips, send_hot, ghost_hot, hot],
        big * cells * FACES * 2, ())
    from_left = shift(right, 1)
    part, near, partial, left = call(
        second_kernel, [whole, pair, f32(1, LANES), slab],
        [image, kappa, faces, nbr, orientation, trace_rest, back_local, weight_rows, flips, hot, send_hot, field],
        big * cells * FACES * 2, ())
    from_right = shift(left, -1)
    sums, edge = call(
        energy_kernel, [f32(devices, LANES), f32(SLAB, cells)],
        [near, faces, kappa, from_left, nbr, orientation, flips, ghost_hot, partial],
        big * SLAB * 2, ())
    sums = lax.all_to_all(sums, AXES, 0, 0, tiled=True)
    total = jnp.sum(sums, axis=0, keepdims=True)
    return tuple(call(
        update_kernel, [f32(BLOCK, cells)] * 2,
        [total, field, image, part, edge, near, faces, kappa, from_right, nbr, orientation, back_ghost, flips,
         ghost_hot], big * 2 * SLAB * 3,
        [pltpu.VMEM((BLOCK, cells), jnp.float32)] * 2 + [pltpu.SemaphoreType.DMA((2,))], out=pltpu.MemorySpace.HBM))


def solution(mesh):
    in_specs = (
        P(None, AXES),
        P(AXES),
        P(AXES),
        P(None, AXES),
        P(None, AXES),
        P(None, AXES),
    )
    out_specs = (P(None, AXES), P(None, AXES))
    return jax.shard_map(body, mesh=mesh, in_specs=in_specs, out_specs=out_specs, check_vma=False)
```

```python
import functools

import jax
import jax.numpy as jnp
import numpy as np
from jax import lax
from jax.experimental import pallas as pl
from jax.experimental.pallas import tpu as pltpu
from jax.sharding import PartitionSpec as P


NODES = 5
FACE = NODES * NODES
BLOCK = NODES**3
MOVE = 64
LANES = 128
ROWS = 128
HALF = 32
SLAB = 2 * HALF
THIN = 56
FACES = 6
PENALTY = 80.0
AXES = ("curve", "group")
VMEM_LIMIT = 24 * 1024 * 1024

GAUSS_POINTS = (-0.906179845938664, -0.5384693101056831, 0.0, 0.5384693101056831, 0.906179845938664)
GAUSS_WEIGHTS = (
    0.2369268850561891,
    0.4786286704993665,
    0.5688888888888889,
    0.4786286704993665,
    0.2369268850561891,
)


def lagrange_value(points, position, location):
    value = 1.0
    for other in range(len(points)):
        if other != position:
            value = value * (location - points[other]) / (points[position] - points[other])
    return value


def lagrange_slope(points, position, location):
    total = 0.0
    for skipped in range(len(points)):
        if skipped == position:
            continue
        addend = 1.0 / (points[position] - points[skipped])
        for other in range(len(points)):
            if other != position and other != skipped:
                addend = addend * (location - points[other]) / (points[position] - points[other])
        total = total + addend
    return total


def basis_tables():
    points = [0.5 * (value + 1.0) for value in GAUSS_POINTS]
    weights = [0.5 * value for value in GAUSS_WEIGHTS]
    count = len(points)
    slopes = [[lagrange_slope(points, p, points[q]) for p in range(count)] for q in range(count)]
    start_value = [lagrange_value(points, p, 0.0) for p in range(count)]
    end_value = [lagrange_value(points, p, 1.0) for p in range(count)]
    start_slope = [-lagrange_slope(points, p, 0.0) for p in range(count)]
    end_slope = [lagrange_slope(points, p, 1.0) for p in range(count)]
    listed = (weights, slopes, start_value, end_value, start_slope, end_slope)
    return [np.asarray(np.asarray(table, np.float32), np.float64) for table in listed]


def along_axis(matrix, axis_id):
    factors = [np.eye(NODES)] * 3
    factors[axis_id] = matrix
    return np.kron(factors[0], np.kron(factors[1], factors[2]))


def parity_basis():
    root = np.sqrt(0.5)
    line = np.zeros((NODES, NODES))
    line[0, 0] = line[0, 4] = line[1, 1] = line[1, 3] = root
    line[2, 2] = 1.0
    line[3, 0], line[3, 4] = root, -root
    line[4, 1], line[4, 3] = root, -root
    odd = np.array([0, 0, 0, 1, 1])
    return np.kron(line, line), np.repeat(odd, NODES), np.tile(odd, NODES)


def split_two(matrix):
    high = matrix.astype(np.float32).astype(jnp.bfloat16)
    low = (matrix - high.astype(np.float64)).astype(np.float32).astype(jnp.bfloat16)
    return high, low


@functools.cache
def operator_constants():
    weights, slopes, *ends = basis_tables()
    cell_weight = np.kron(weights, np.kron(weights, weights))
    face_weight = np.kron(weights, weights)
    parity, odd_first, odd_second = parity_basis()
    stiff = np.zeros((BLOCK, BLOCK))
    for axis_id in range(3):
        grad = along_axis(slopes, axis_id)
        stiff += grad.T @ (cell_weight[:, None] * grad)
    trace = np.zeros((FACES * SLAB + ROWS, ROWS))
    back = np.zeros((ROWS, FACES * SLAB))
    for face in range(FACES):
        tangent = along_axis(ends[face % 2][None, :], face // 2)
        normal = along_axis(ends[2 + face % 2][None, :], face // 2)
        start = face * SLAB
        trace[start : start + FACE, :BLOCK] = parity @ tangent
        trace[start + HALF : start + HALF + FACE, :BLOCK] = parity @ normal
        spread = (face_weight[:, None] * parity.T)
        back[:BLOCK, start : start + FACE] = tangent.T @ spread
        back[:BLOCK, start + HALF : start + HALF + FACE] = -0.5 * normal.T @ spread
    trace[FACES * SLAB : FACES * SLAB + BLOCK, :BLOCK] = stiff
    high, low = split_two(trace)
    trace3 = np.concatenate([high, high, low], 1)
    trace_pair, trace_rest = trace3[: 2 * SLAB], trace3[2 * SLAB :]
    backs = []
    for first, last in ((0, 2), (2, FACES)):
        high, low = split_two(back[:, first * SLAB : last * SLAB])
        backs.append(np.concatenate([high, high, low], 1))
    weight_rows = np.zeros((ROWS, 1), np.float32)
    weight_rows[:BLOCK, 0] = cell_weight
    flips = np.zeros((SLAB, LANES), np.float32)
    for start in (0, HALF):
        flips[start : start + FACE, 0] = odd_first
        flips[start : start + FACE, 1] = odd_second
        flips[start : start + FACE, 2] = np.diag(parity @ (face_weight[:, None] * parity.T))
    return trace_pair, trace_rest, backs[0], backs[1], weight_rows, flips


def as_bf16(value):
    return value.astype(jnp.bfloat16)


def as_f32(value):
    return value.astype(jnp.float32)


def parts_of(value, count):
    pieces = []
    for step in range(count):
        piece = as_bf16(value)
        pieces.append(piece)
        if step + 1 < count:
            value = value - as_f32(piece)
    return pieces


def dot(left, right):
    return lax.dot_general(left, right, (((1,), (0,)), ((), ())), preferred_element_type=jnp.float32)


def dot_rows(left, right):
    return lax.dot_general(left, right, (((1,), (1,)), ((), ())), preferred_element_type=jnp.float32)


def times3(table3, value):
    high, low = parts_of(value, 2)
    return dot(table3, jnp.concatenate([high, low, high], 0))


def pick(value, chosen, count):
    rows = value.shape[0]
    out = dot(jnp.concatenate(parts_of(value, count), 0), chosen)
    total = out[(count - 1) * rows :]
    for step in reversed(range(count - 1)):
        total = total + out[step * rows : (step + 1) * rows]
    return total


def one_hot(index_row, rows, offset=0):
    ids = lax.broadcasted_iota(jnp.int32, (rows, index_row.shape[1]), 0)
    return as_bf16(jnp.where(ids == index_row - offset, 1.0, 0.0))


def call(kernel, outs, args, flops, scratch=(), far=0, out=pltpu.VMEM):
    moved = sum(a.size * a.dtype.itemsize for a in args) + sum(o.size * o.dtype.itemsize for o in outs)
    spaces = [pltpu.MemorySpace.HBM] * far + [pltpu.VMEM] * (len(args) - far)
    args = [pltpu.with_memory_space_constraint(a, pltpu.MemorySpace.HBM) if i < far else a
            for i, a in enumerate(args)]
    return pl.pallas_call(
        kernel,
        out_shape=list(outs),
        in_specs=[pl.BlockSpec(memory_space=space) for space in spaces],
        out_specs=[pl.BlockSpec(memory_space=out) for _ in outs],
        scratch_shapes=list(scratch),
        compiler_params=pltpu.CompilerParams(vmem_limit_bytes=VMEM_LIMIT),
        cost_estimate=pl.CostEstimate(flops=flops, bytes_accessed=moved, transcendentals=0),
    )(*args)


def f32(*shape):
    return jax.ShapeDtypeStruct(shape, jnp.float32)


def my_rank():
    return lax.axis_index("curve") * lax.axis_size("group") + lax.axis_index("group")


def pack_kernel(rhs_hbm, cond_hbm, dest_hbm, send_hbm, trace_hbm, nbr_hbm, near_up_ref, near_down_ref, far_up_ref,
                far_down_ref, packed_ref, payload_ref, stay_ref, send, nbr, trace, rhs, cond, dest_row, sems):
    cells = dest_row.shape[1]
    tiles = cells // LANES
    copies = [
        pltpu.make_async_copy(source, target, sems.at[place])
        for place, (source, target) in enumerate(
            ((dest_hbm, dest_row), (send_hbm, send), (cond_hbm, cond), (rhs_hbm, rhs), (trace_hbm, trace),
             (nbr_hbm, nbr))
        )
    ]
    for copy in copies:
        copy.start()
    copies[0].wait()
    copies[1].wait()
    dest = dest_row[...]
    owner = lax.div(dest, cells)
    target, slot = owner - my_rank(), dest - owner * cells
    stay = jnp.where(target == 0, slot, -1)
    stay_ref[...] = stay
    leaving = [target == -1, target == 1]
    marks = [as_f32(mask) for mask in leaving]
    stacked = jnp.concatenate(
        [mark[:, t * LANES : (t + 1) * LANES] for mark in marks for t in range(tiles)], 0
    )
    first = lax.broadcasted_iota(jnp.int32, (LANES, LANES), 0)
    second = lax.broadcasted_iota(jnp.int32, (LANES, LANES), 1)
    counts = dot(as_bf16(stacked), as_bf16(jnp.where(first <= second, 1.0, 0.0)))
    places = []
    for side in range(2):
        base = jnp.zeros((1, 1), jnp.float32)
        line = []
        for t in range(tiles):
            row = counts[side * tiles + t : side * tiles + t + 1]
            line.append(row + base)
            base = base + row[:, LANES - 1 :]
        places.append(jnp.concatenate(line, 1).astype(jnp.int32) - 1)
    place = jnp.where(leaving[0], places[0], jnp.where(leaving[1], MOVE + places[1], -1))
    chosen = one_hot(place, 2 * MOVE)
    lists = as_f32(send[...])
    columns = jnp.concatenate([lists, jnp.zeros((6, lists.shape[1]), jnp.float32)], 0).T
    stay_row = as_f32(stay)
    kept = [as_bf16(jnp.where(columns[:, side : side + 1] == stay_row, 1.0, 0.0)) for side in range(2)]
    for copy in copies[2:]:
        copy.wait()
    payload_ref[:BLOCK] = rhs[...]
    payload_ref[BLOCK : BLOCK + 1] = cond[...]
    payload_ref[BLOCK + 1 : BLOCK + 2] = as_f32(slot + 1)
    payload_ref[BLOCK + 2 : ROWS] = jnp.zeros((ROWS - BLOCK - 2, cells), jnp.float32)
    payload = payload_ref[...]
    out = dot_rows(chosen, jnp.concatenate(parts_of(payload, 2), 0))
    packed = out[:, :ROWS] + out[:, ROWS:]
    packed_ref[...] = packed
    traces = face_rows(times3(trace[...], payload), cond[...], 2)
    sides = []
    for side in range(2):
        out = dot_rows(jnp.concatenate(parts_of(traces[side], 2), 0), kept[side])
        ghosts = out[:SLAB] + out[SLAB:]
        row = lax.broadcasted_iota(jnp.int32, (SLAB, 1), 0)
        ghosts = jnp.where(row == FACE + 1, lists[side : side + 1] + 1.0, ghosts)
        moving = packed[side * MOVE : (side + 1) * MOVE]
        half = MOVE // 2
        sides.append(jnp.concatenate([ghosts, jnp.concatenate([moving[:half], moving[half:]], 1)], 0))
    near_up_ref[...] = sides[1]
    near_down_ref[...] = sides[0]
    far_up_ref[...] = packed[MOVE:]
    far_down_ref[...] = packed[:MOVE]


def stay_kernel(count, *refs):
    far, (payload_ref, stay_ref, send_ref, neighbour_ref, pair_trace_ref) = refs[:count], refs[count : count + 5]
    placed_ref, send_hot_ref, ghost_hot_ref, hot_ref, slab_ref, beside_ref, stiff_ref = refs[count + 5 : count + 12]
    close, sems = refs[count + 12 : -1], refs[-1]
    copies = [pltpu.make_async_copy(far[k], close[k], sems.at[k]) for k in range(count)]
    for copy in copies:
        copy.start()
    cells = stay_ref.shape[1]
    ghosts = send_ref.shape[1]
    out = dot_rows(jnp.concatenate(parts_of(payload_ref[...], 3), 0), one_hot(stay_ref[...], cells))
    placed = out[:ROWS] + (out[ROWS : 2 * ROWS] + out[2 * ROWS :])
    placed_ref[...] = placed
    for side in range(2):
        send_hot_ref[side] = one_hot(send_ref[side : side + 1], cells)
        ghost_hot_ref[side] = one_hot(neighbour_ref[side : side + 1], ghosts, cells + side * ghosts)
    for face in range(FACES):
        hot_ref[face] = one_hot(neighbour_ref[face : face + 1], cells)
    for copy in copies:
        copy.wait()
    slabs, stiff = all_faces(placed, placed[BLOCK : BLOCK + 1], pair_trace_ref, close[1])
    stiff_ref[...] = stiff
    for face in range(FACES):
        slab_ref[face * SLAB : (face + 1) * SLAB] = slabs[face]
        beside_ref[face * SLAB : (face + 1) * SLAB] = pick(slabs[face ^ 1], hot_ref[face], 2)


def face_rows(out, kappa, count):
    row = lax.broadcasted_iota(jnp.int32, (HALF, 1), 0)
    slabs = []
    for face in range(count):
        start = face * SLAB
        values = jnp.where(row == FACE, kappa, out[start : start + HALF])
        slabs.append(jnp.concatenate([values, kappa * out[start + HALF : start + SLAB]], 0))
    return slabs


def all_faces(field, kappa, pair_trace_ref, trace_ref):
    high, low = parts_of(field, 2)
    triple = jnp.concatenate([high, low, high], 0)
    out = dot(trace_ref[...], triple)
    slabs = face_rows(dot(pair_trace_ref[...], triple), kappa, 2) + face_rows(out, kappa, FACES - 2)
    return slabs, kappa * out[(FACES - 2) * SLAB :]


def moved_ghosts(records, lists, trace_ref):
    columns = records.T
    slabs = face_rows(times3(trace_ref[...], columns), columns[BLOCK : BLOCK + 1], 2)
    slots = records[:, BLOCK + 1 : BLOCK + 2]
    side_of = lax.broadcasted_iota(jnp.int32, (2 * MOVE, 1), 0) // MOVE
    found = []
    for side in range(2):
        wanted = jnp.where(side_of == side, slots, -1.0)
        found.append(pick(slabs[1 - side], as_bf16(jnp.where(wanted == lists[side], 1.0, 0.0)), 2))
    return found


def face_jumps(face, near, own, kappa, neighbour_ref, code_ref, flips):
    code = code_ref[face : face + 1]
    first = 1.0 - 2.0 * as_f32(jnp.bitwise_and(code, 1))
    second = 1.0 - 2.0 * as_f32(jnp.right_shift(code, 1))
    sign = jnp.where(flips[:HALF, 0:1] > 0.0, first, 1.0) * jnp.where(flips[:HALF, 1:2] > 0.0, second, 1.0)
    outside = jnp.where(neighbour_ref[face : face + 1] < 0, 2.0, 1.0)
    strength = PENALTY * jnp.maximum(kappa, near[FACE : FACE + 1])
    values = outside * own[:HALF] - sign * near[:HALF]
    return values, outside * own[HALF:] - sign * near[HALF:], strength


def face_terms(jumps, kappa):
    values, fluxes, strength = jumps
    return jnp.concatenate([strength * values - 0.5 * fluxes, kappa * values], 0)


def one_sided(jumps, own):
    values, fluxes, strength = jumps
    return own[:HALF] * (strength * values - 0.5 * fluxes) - 0.5 * own[HALF:] * values


def both_sided(jumps):
    values, fluxes, strength = jumps
    return values * (strength * values - fluxes)


def first_kernel(placed_ref, slab_ref, beside_ref, stiff_ref, near_up_ref, near_down_ref, far_up_ref, far_down_ref, packed_ref, pair_trace_ref,
                 neighbour_ref, code_ref, trace_ref, back_ref, back_ghost_ref, weight_ref, flip_ref, send_hot_ref,
                 ghost_hot_ref, field_ref, kappa_ref, image_ref, pair_ref, right_ref):
    cells = placed_ref.shape[1]
    buffers = (near_up_ref[...], near_down_ref[...])
    records = jnp.concatenate(
        [piece for buffer in buffers for piece in (buffer[SLAB:, :LANES], buffer[SLAB:, LANES:])], 0
    )
    slot = records[:, BLOCK + 1 : BLOCK + 2].astype(jnp.int32) - 1
    slot = jnp.where(slot < 0, -2, slot)
    ids = lax.broadcasted_iota(jnp.int32, (2 * MOVE, cells), 1)
    arrived = records.T
    new_slabs, new_stiff = all_faces(arrived, arrived[BLOCK : BLOCK + 1], pair_trace_ref, trace_ref)
    added = pick(jnp.concatenate([*new_slabs, new_stiff, arrived], 0), as_bf16(jnp.where(ids == slot, 1.0, 0.0)), 2)
    merged = placed_ref[...] + added[FACES * SLAB + ROWS :]
    kappa = merged[BLOCK : BLOCK + 1]
    row = lax.broadcasted_iota(jnp.int32, (ROWS, 1), 0)
    field = jnp.where(row < BLOCK, merged, 0.0)
    field_ref[...] = field
    kappa_ref[...] = kappa
    slabs = [
        slab_ref[face * SLAB : (face + 1) * SLAB] + added[face * SLAB : (face + 1) * SLAB] for face in range(FACES)
    ]
    stiff = stiff_ref[...] + added[FACES * SLAB : FACES * SLAB + ROWS]
    lists = [buffer[FACE + 1 : FACE + 2] for buffer in buffers]
    far = jnp.concatenate([far_up_ref[...], far_down_ref[...]], 0)
    moved = [moved_ghosts(some, lists, pair_trace_ref) for some in (packed_ref[...], far)]
    flips = flip_ref[...]
    terms = []
    for face in range(FACES):
        chosen = as_bf16(jnp.where(slot == neighbour_ref[face : face + 1], 1.0, 0.0))
        near = beside_ref[face * SLAB : (face + 1) * SLAB] + pick(new_slabs[face ^ 1], chosen, 2)
        if face < 2:
            ghosts = buffers[face][:SLAB] + (moved[0][face] + moved[1][face])
            near = near + pick(ghosts, ghost_hot_ref[face], 2)
        jumps = face_jumps(face, near, slabs[face], kappa, neighbour_ref, code_ref, flips)
        terms.append(face_terms(jumps, kappa))
    volume = weight_ref[...] * field + stiff
    image = (volume + times3(back_ref[...], jnp.concatenate(terms[2:], 0))
             + times3(back_ghost_ref[...], jnp.concatenate(terms[:2], 0)))
    image_ref[...] = image
    pair_ref[:SLAB], pair_ref[SLAB:] = face_rows(times3(pair_trace_ref[...], image), kappa, 2)
    right_ref[...] = squeeze(pick(pair_ref[SLAB:], send_hot_ref[1], 2))


def whole_sum(value):
    return jnp.sum(jnp.sum(value, axis=0, keepdims=True), axis=1, keepdims=True)


def second_kernel(image_ref, kappa_ref, pair_ref, neighbour_ref, code_ref, trace_ref, back_ref, weight_ref,
                  flip_ref, hot_ref, send_hot_ref, field_ref, part_ref, near_ref, sums_ref, left_ref):
    left_ref[...] = squeeze(pick(pair_ref[:SLAB], send_hot_ref[0], 2))
    cells = image_ref.shape[1]
    kappa = kappa_ref[...]
    flips = flip_ref[...]
    field, image = field_ref[...], image_ref[...]
    out = times3(trace_ref[...], image)
    slabs = face_rows(out, kappa, FACES - 2)
    total = jnp.zeros((HALF, cells), jnp.float32)
    terms = []
    for face in range(FACES):
        slab = pair_ref[(1 - face) * SLAB : (2 - face) * SLAB] if face < 2 else slabs[(face ^ 1) - 2]
        near = pick(slab, hot_ref[face], 2)
        if face < 2:
            near_ref[face * SLAB : (face + 1) * SLAB] = near
        if face == 0:
            continue
        own = pair_ref[SLAB:] if face == 1 else slabs[face - 2]
        jumps = face_jumps(face, near, own, kappa, neighbour_ref, code_ref, flips)
        share = one_sided(jumps, own)
        if face == 1:
            total = total + jnp.where(neighbour_ref[1:2] < cells, share, 0.0)
        else:
            total = total + share
            terms.append(face_terms(jumps, kappa))
    volume = weight_ref[...] * image + kappa * out[(FACES - 2) * SLAB :]
    part_ref[...] = volume + times3(back_ref[...], jnp.concatenate(terms, 0))
    totals = (whole_sum(field * field), whole_sum(field * image), whole_sum(image * image),
              whole_sum(image * volume) + whole_sum(flips[:HALF, 2:3] * total))
    lane = lax.broadcasted_iota(jnp.int32, (1, LANES), 1)
    sums = jnp.zeros((1, LANES), jnp.float32)
    for place, value in enumerate(totals):
        sums = jnp.where(lane == place, value, sums)
    sums_ref[...] = sums


def squeeze(slab):
    idle = jnp.zeros((THIN - 2 * FACE - 1, slab.shape[1]), jnp.float32)
    return jnp.concatenate([slab[: FACE + 1], slab[HALF : HALF + FACE], idle], 0)


def spread(thin):
    gap = jnp.zeros((HALF - FACE - 1, thin.shape[1]), jnp.float32)
    tail = jnp.zeros((HALF - FACE, thin.shape[1]), jnp.float32)
    return jnp.concatenate([thin[: FACE + 1], gap, thin[FACE + 1 : 2 * FACE + 1], tail], 0)


def ghost_jumps(face, ghosts, near_ref, pair_ref, kappa, neighbour_ref, code_ref, flips, ghost_hot_ref):
    rows = slice(face * SLAB, (face + 1) * SLAB)
    near = near_ref[rows] + pick(ghosts, ghost_hot_ref[face], 2)
    return face_jumps(face, near, pair_ref[rows], kappa, neighbour_ref, code_ref, flips)


def energy_kernel(near_ref, pair_ref, kappa_ref, from_left_ref, neighbour_ref, code_ref, flip_ref,
                  ghost_hot_ref, partial_ref, sums_ref, term_ref):
    cells = near_ref.shape[1]
    kappa = kappa_ref[...]
    flips = flip_ref[...]
    jumps = ghost_jumps(0, spread(from_left_ref[...]), near_ref, pair_ref, kappa, neighbour_ref, code_ref, flips,
                        ghost_hot_ref)
    term_ref[...] = face_terms(jumps, kappa)
    shared = jnp.where(neighbour_ref[0:1] < cells, one_sided(jumps, pair_ref[:SLAB]), both_sided(jumps))
    total = whole_sum(flips[:HALF, 2:3] * shared)
    lane = lax.broadcasted_iota(jnp.int32, (1, LANES), 1)
    sums = partial_ref[...] + jnp.where(lane == 3, total, 0.0)
    sums_ref[...] = jnp.broadcast_to(sums, sums_ref.shape)


def update_kernel(sums_ref, field_ref, image_ref, part_ref, edge_ref, near_ref, pair_ref, kappa_ref,
                  from_right_ref, neighbour_ref, code_ref, back_ref, flip_ref, ghost_hot_ref,
                  solution_hbm, residual_hbm, solution, residual, sems):
    sums = sums_ref[...]
    bb, bw, ww, wt = (sums[:, place : place + 1] for place in range(4))
    alpha = bb / bw
    rr = bb - 2.0 * alpha * bw + alpha * alpha * ww
    beta = rr / bb
    more = 1.0 + beta
    inner = more * more * bw - 2.0 * alpha * more * ww + alpha * alpha * wt
    step = rr / inner
    field, image = field_ref[:BLOCK], image_ref[:BLOCK]
    solution[...] = (alpha + step * more) * field - (step * alpha) * image
    first = pltpu.make_async_copy(solution, solution_hbm, sems.at[0])
    first.start()
    kappa = kappa_ref[...]
    jumps = ghost_jumps(1, spread(from_right_ref[...]), near_ref, pair_ref, kappa, neighbour_ref, code_ref,
                        flip_ref[...], ghost_hot_ref)
    edges = jnp.concatenate([edge_ref[...], face_terms(jumps, kappa)], 0)
    twice = part_ref[...] + times3(back_ref[...], edges)
    residual[...] = field - (alpha + step * more) * image + (step * alpha) * twice[:BLOCK]
    second = pltpu.make_async_copy(residual, residual_hbm, sems.at[1])
    second.start()
    first.wait()
    second.wait()


def shift(value, distance):
    count = lax.axis_size(AXES)
    return lax.ppermute(value, AXES, [(i, (i + distance) % count) for i in range(count)])


def bf16(*shape):
    return jax.ShapeDtypeStruct(shape, jnp.bfloat16)


def i32(*shape):
    return jax.ShapeDtypeStruct(shape, jnp.int32)


def body(right_side, conductivity, destination, neighbour, orientation, send_list):
    constants = (jnp.asarray(table) for table in operator_constants())
    trace_pair, trace_rest, back_ghost, back_local, weight_rows, flips = constants
    devices = lax.axis_size(AXES)
    cells = destination.shape[0]
    ghosts = send_list.shape[1]
    whole, slab, row = f32(ROWS, cells), f32(THIN, ghosts), f32(1, cells)
    pair = f32(2 * SLAB, cells)
    big = 2 * ROWS * cells
    near_up, near_down, far_up, far_down, packed, payload, stay, send, nbr, trace_pair = call(
        pack_kernel,
        [f32(SLAB + MOVE // 2, ghosts)] * 2 + [f32(MOVE, ROWS)] * 2
        + [f32(2 * MOVE, ROWS), whole, i32(1, cells), i32(2, ghosts), i32(FACES, cells), bf16(*trace_pair.shape)],
        [right_side, conductivity[None], destination[None], send_list, trace_pair, neighbour], big * LANES * 6,
        [pltpu.VMEM((BLOCK, cells), jnp.float32), pltpu.VMEM((1, cells), jnp.float32),
         pltpu.VMEM((1, cells), jnp.int32), pltpu.SemaphoreType.DMA((6,))],
        far=6)
    near_up = shift(near_up, 1)
    far_up = shift(far_up, 2)
    far_down = shift(far_down, -2)
    near_down = shift(near_down, -1)
    later = [orientation, trace_rest, back_local, back_ghost, weight_rows, flips]
    slabs = f32(FACES * SLAB, cells)
    placed, send_hot, ghost_hot, hot, slab_rows, beside, stiff, *later = call(
        functools.partial(stay_kernel, len(later)),
        [whole, bf16(2, cells, ghosts), bf16(2, ghosts, cells), bf16(FACES, cells, cells), slabs, slabs, whole]
        + [jax.ShapeDtypeStruct(a.shape, a.dtype) for a in later],
        later + [payload, stay, send, nbr, trace_pair], big * cells * 3, [pltpu.SemaphoreType.DMA((len(later),))],
        far=len(later))
    orientation, trace_rest, back_local, back_ghost, weight_rows, flips = later
    field, kappa, image, faces, right = call(
        first_kernel, [whole, row, whole, pair, slab],
        [placed, slab_rows, beside, stiff, near_up, near_down, far_up, far_down, packed, trace_pair, nbr, orientation, trace_rest,
         back_local, back_ghost, weight_rows, flips, send_hot, ghost_hot],
        big * cells * FACES * 2, ())
    from_left = shift(right, 1)
    part, near, partial, left = call(
        second_kernel, [whole, pair, f32(1, LANES), slab],
        [image, kappa, faces, nbr, orientation, trace_rest, back_local, weight_rows, flips, hot, send_hot, field],
        big * cells * FACES * 2, ())
    from_right = shift(left, -1)
    sums, edge = call(
        energy_kernel, [f32(devices, LANES), f32(SLAB, cells)],
        [near, faces, kappa, from_left, nbr, orientation, flips, ghost_hot, partial],
        big * SLAB * 2, ())
    sums = lax.all_to_all(sums, AXES, 0, 0, tiled=True)
    total = jnp.sum(sums, axis=0, keepdims=True)
    return tuple(call(
        update_kernel, [f32(BLOCK, cells)] * 2,
        [total, field, image, part, edge, near, faces, kappa, from_right, nbr, orientation, back_ghost, flips,
         ghost_hot], big * 2 * SLAB * 3,
        [pltpu.VMEM((BLOCK, cells), jnp.float32)] * 2 + [pltpu.SemaphoreType.DMA((2,))], out=pltpu.MemorySpace.HBM))


def solution(mesh):
    in_specs = (
        P(None, AXES),
        P(AXES),
        P(AXES),
        P(None, AXES),
        P(None, AXES),
        P(None, AXES),
    )
    out_specs = (P(None, AXES), P(None, AXES))
    return jax.shard_map(body, mesh=mesh, in_specs=in_specs, out_specs=out_specs, check_vma=False)
```

```python
import functools

import jax
import jax.numpy as jnp
import numpy as np
from jax import lax
from jax.experimental import pallas as pl
from jax.experimental.pallas import tpu as pltpu
from jax.sharding import PartitionSpec as P


NODES = 5
FACE = NODES * NODES
BLOCK = NODES**3
MOVE = 64
LANES = 128
ROWS = 128
HALF = 32
SLAB = 2 * HALF
THIN = 56
LIST = 2 * FACE + 1
FACES = 6
PENALTY = 80.0
AXES = ("curve", "group")
VMEM_LIMIT = 24 * 1024 * 1024

GAUSS_POINTS = (-0.906179845938664, -0.5384693101056831, 0.0, 0.5384693101056831, 0.906179845938664)
GAUSS_WEIGHTS = (
    0.2369268850561891,
    0.4786286704993665,
    0.5688888888888889,
    0.4786286704993665,
    0.2369268850561891,
)


def lagrange_value(points, position, location):
    value = 1.0
    for other in range(len(points)):
        if other != position:
            value = value * (location - points[other]) / (points[position] - points[other])
    return value


def lagrange_slope(points, position, location):
    total = 0.0
    for skipped in range(len(points)):
        if skipped == position:
            continue
        addend = 1.0 / (points[position] - points[skipped])
        for other in range(len(points)):
            if other != position and other != skipped:
                addend = addend * (location - points[other]) / (points[position] - points[other])
        total = total + addend
    return total


def basis_tables():
    points = [0.5 * (value + 1.0) for value in GAUSS_POINTS]
    weights = [0.5 * value for value in GAUSS_WEIGHTS]
    count = len(points)
    slopes = [[lagrange_slope(points, p, points[q]) for p in range(count)] for q in range(count)]
    start_value = [lagrange_value(points, p, 0.0) for p in range(count)]
    end_value = [lagrange_value(points, p, 1.0) for p in range(count)]
    start_slope = [-lagrange_slope(points, p, 0.0) for p in range(count)]
    end_slope = [lagrange_slope(points, p, 1.0) for p in range(count)]
    listed = (weights, slopes, start_value, end_value, start_slope, end_slope)
    return [np.asarray(np.asarray(table, np.float32), np.float64) for table in listed]


def along_axis(matrix, axis_id):
    factors = [np.eye(NODES)] * 3
    factors[axis_id] = matrix
    return np.kron(factors[0], np.kron(factors[1], factors[2]))


def parity_basis():
    root = np.sqrt(0.5)
    line = np.zeros((NODES, NODES))
    line[0, 0] = line[0, 4] = line[1, 1] = line[1, 3] = root
    line[2, 2] = 1.0
    line[3, 0], line[3, 4] = root, -root
    line[4, 1], line[4, 3] = root, -root
    odd = np.array([0, 0, 0, 1, 1])
    return np.kron(line, line), np.repeat(odd, NODES), np.tile(odd, NODES)


def split_two(matrix):
    high = matrix.astype(np.float32).astype(jnp.bfloat16)
    low = (matrix - high.astype(np.float64)).astype(np.float32).astype(jnp.bfloat16)
    return high, low


@functools.cache
def operator_constants():
    weights, slopes, *ends = basis_tables()
    cell_weight = np.kron(weights, np.kron(weights, weights))
    face_weight = np.kron(weights, weights)
    parity, odd_first, odd_second = parity_basis()
    stiff = np.zeros((BLOCK, BLOCK))
    for axis_id in range(3):
        grad = along_axis(slopes, axis_id)
        stiff += grad.T @ (cell_weight[:, None] * grad)
    trace = np.zeros((FACES * SLAB + ROWS, ROWS))
    back = np.zeros((ROWS, FACES * SLAB))
    for face in range(FACES):
        tangent = along_axis(ends[face % 2][None, :], face // 2)
        normal = along_axis(ends[2 + face % 2][None, :], face // 2)
        start = face * SLAB
        trace[start : start + FACE, :BLOCK] = parity @ tangent
        trace[start + HALF : start + HALF + FACE, :BLOCK] = parity @ normal
        spread = (face_weight[:, None] * parity.T)
        back[:BLOCK, start : start + FACE] = tangent.T @ spread
        back[:BLOCK, start + HALF : start + HALF + FACE] = -0.5 * normal.T @ spread
    trace[FACES * SLAB : FACES * SLAB + BLOCK, :BLOCK] = stiff
    high, low = split_two(trace)
    trace3 = np.concatenate([high, high, low], 1)
    trace_pair, trace_rest = trace3[: 2 * SLAB], trace3[2 * SLAB :]
    backs = []
    for first, last in ((0, 2), (2, FACES)):
        high, low = split_two(back[:, first * SLAB : last * SLAB])
        backs.append(np.concatenate([high, high, low], 1))
    weight_rows = np.zeros((ROWS, 1), np.float32)
    weight_rows[:BLOCK, 0] = cell_weight
    flips = np.zeros((SLAB, LANES), np.float32)
    for start in (0, HALF):
        flips[start : start + FACE, 0] = odd_first
        flips[start : start + FACE, 1] = odd_second
        flips[start : start + FACE, 2] = np.diag(parity @ (face_weight[:, None] * parity.T))
    return trace_pair, trace_rest, backs[0], backs[1], weight_rows, flips


def as_bf16(value):
    return value.astype(jnp.bfloat16)


def as_f32(value):
    return value.astype(jnp.float32)


def parts_of(value, count):
    pieces = []
    for step in range(count):
        piece = as_bf16(value)
        pieces.append(piece)
        if step + 1 < count:
            value = value - as_f32(piece)
    return pieces


def dot(left, right):
    return lax.dot_general(left, right, (((1,), (0,)), ((), ())), preferred_element_type=jnp.float32)


def dot_rows(left, right):
    return lax.dot_general(left, right, (((1,), (1,)), ((), ())), preferred_element_type=jnp.float32)


def times3(table3, value):
    high, low = parts_of(value, 2)
    return dot(table3, jnp.concatenate([high, low, high], 0))


def pick(value, chosen, count):
    rows = value.shape[0]
    out = dot(jnp.concatenate(parts_of(value, count), 0), chosen)
    total = out[(count - 1) * rows :]
    for step in reversed(range(count - 1)):
        total = total + out[step * rows : (step + 1) * rows]
    return total


def one_hot(index_row, rows, offset=0):
    ids = lax.broadcasted_iota(jnp.int32, (rows, index_row.shape[1]), 0)
    return as_bf16(jnp.where(ids == index_row - offset, 1.0, 0.0))


def call(kernel, outs, args, flops, scratch=(), far=0, out=pltpu.VMEM):
    moved = sum(a.size * a.dtype.itemsize for a in args) + sum(o.size * o.dtype.itemsize for o in outs)
    spaces = [pltpu.MemorySpace.HBM] * far + [pltpu.VMEM] * (len(args) - far)
    args = [pltpu.with_memory_space_constraint(a, pltpu.MemorySpace.HBM) if i < far else a
            for i, a in enumerate(args)]
    return pl.pallas_call(
        kernel,
        out_shape=list(outs),
        in_specs=[pl.BlockSpec(memory_space=space) for space in spaces],
        out_specs=[pl.BlockSpec(memory_space=out) for _ in outs],
        scratch_shapes=list(scratch),
        compiler_params=pltpu.CompilerParams(vmem_limit_bytes=VMEM_LIMIT),
        cost_estimate=pl.CostEstimate(flops=flops, bytes_accessed=moved, transcendentals=0),
    )(*args)


def f32(*shape):
    return jax.ShapeDtypeStruct(shape, jnp.float32)


def my_rank():
    return lax.axis_index("curve") * lax.axis_size("group") + lax.axis_index("group")


def pack_kernel(rhs_hbm, cond_hbm, dest_hbm, send_hbm, trace_hbm, nbr_hbm, near_up_ref, near_down_ref, far_up_ref,
                far_down_ref, packed_ref, payload_ref, stay_ref, send, nbr, trace, rhs, cond, dest_row, sems):
    cells = dest_row.shape[1]
    tiles = cells // LANES
    copies = [
        pltpu.make_async_copy(source, target, sems.at[place])
        for place, (source, target) in enumerate(
            ((dest_hbm, dest_row), (send_hbm, send), (cond_hbm, cond), (rhs_hbm, rhs), (trace_hbm, trace),
             (nbr_hbm, nbr))
        )
    ]
    for copy in copies:
        copy.start()
    copies[0].wait()
    copies[1].wait()
    dest = dest_row[...]
    owner = lax.div(dest, cells)
    target, slot = owner - my_rank(), dest - owner * cells
    stay = jnp.where(target == 0, slot, -1)
    stay_ref[...] = stay
    leaving = [target == -1, target == 1]
    marks = [as_f32(mask) for mask in leaving]
    stacked = jnp.concatenate(
        [mark[:, t * LANES : (t + 1) * LANES] for mark in marks for t in range(tiles)], 0
    )
    first = lax.broadcasted_iota(jnp.int32, (LANES, LANES), 0)
    second = lax.broadcasted_iota(jnp.int32, (LANES, LANES), 1)
    counts = dot(as_bf16(stacked), as_bf16(jnp.where(first <= second, 1.0, 0.0)))
    places = []
    for side in range(2):
        base = jnp.zeros((1, 1), jnp.float32)
        line = []
        for t in range(tiles):
            row = counts[side * tiles + t : side * tiles + t + 1]
            line.append(row + base)
            base = base + row[:, LANES - 1 :]
        places.append(jnp.concatenate(line, 1).astype(jnp.int32) - 1)
    place = jnp.where(leaving[0], places[0], jnp.where(leaving[1], MOVE + places[1], -1))
    chosen = one_hot(place, 2 * MOVE)
    lists = as_f32(send[...])
    columns = jnp.concatenate([lists, jnp.zeros((6, lists.shape[1]), jnp.float32)], 0).T
    stay_row = as_f32(stay)
    kept = [as_bf16(jnp.where(columns[:, side : side + 1] == stay_row, 1.0, 0.0)) for side in range(2)]
    for copy in copies[2:]:
        copy.wait()
    payload_ref[:BLOCK] = rhs[...]
    payload_ref[BLOCK : BLOCK + 1] = cond[...]
    payload_ref[BLOCK + 1 : BLOCK + 2] = as_f32(slot + 1)
    payload_ref[BLOCK + 2 : ROWS] = jnp.zeros((ROWS - BLOCK - 2, cells), jnp.float32)
    payload = payload_ref[...]
    out = dot_rows(chosen, jnp.concatenate(parts_of(payload, 2), 0))
    packed = out[:, :ROWS] + out[:, ROWS:]
    packed_ref[...] = packed
    traces = face_rows(times3(trace[...], payload), cond[...], 2)
    sides = []
    for side in range(2):
        out = dot_rows(jnp.concatenate(parts_of(traces[side], 2), 0), kept[side])
        ghosts = out[:SLAB] + out[SLAB:]
        row = lax.broadcasted_iota(jnp.int32, (THIN, 1), 0)
        ghosts = jnp.where(row == LIST, lists[side : side + 1] + 1.0, squeeze(ghosts))
        moving = packed[side * MOVE : (side + 1) * MOVE]
        half = MOVE // 2
        sides.append(jnp.concatenate([ghosts, jnp.concatenate([moving[:half], moving[half:]], 1)], 0))
    near_up_ref[...] = sides[1]
    near_down_ref[...] = sides[0]
    far_up_ref[...] = packed[MOVE:]
    far_down_ref[...] = packed[:MOVE]


def stay_kernel(count, *refs):
    far, (payload_ref, stay_ref, send_ref, neighbour_ref, pair_trace_ref) = refs[:count], refs[count : count + 5]
    placed_ref, send_hot_ref, ghost_hot_ref, hot_ref, slab_ref, beside_ref, stiff_ref = refs[count + 5 : count + 12]
    close, sems = refs[count + 12 : -1], refs[-1]
    copies = [pltpu.make_async_copy(far[k], close[k], sems.at[k]) for k in range(count)]
    for copy in copies:
        copy.start()
    cells = stay_ref.shape[1]
    ghosts = send_ref.shape[1]
    out = dot_rows(jnp.concatenate(parts_of(payload_ref[...], 3), 0), one_hot(stay_ref[...], cells))
    placed = out[:ROWS] + (out[ROWS : 2 * ROWS] + out[2 * ROWS :])
    placed_ref[...] = placed
    for side in range(2):
        send_hot_ref[side] = one_hot(send_ref[side : side + 1], cells)
        ghost_hot_ref[side] = one_hot(neighbour_ref[side : side + 1], ghosts, cells + side * ghosts)
    for face in range(FACES):
        hot_ref[face] = one_hot(neighbour_ref[face : face + 1], cells)
    for copy in copies:
        copy.wait()
    slabs, stiff = all_faces(placed, placed[BLOCK : BLOCK + 1], pair_trace_ref, close[1])
    stiff_ref[...] = stiff
    for face in range(FACES):
        slab_ref[face * SLAB : (face + 1) * SLAB] = slabs[face]
        beside_ref[face * SLAB : (face + 1) * SLAB] = pick(slabs[face ^ 1], hot_ref[face], 2)


def face_rows(out, kappa, count):
    row = lax.broadcasted_iota(jnp.int32, (HALF, 1), 0)
    slabs = []
    for face in range(count):
        start = face * SLAB
        values = jnp.where(row == FACE, kappa, out[start : start + HALF])
        slabs.append(jnp.concatenate([values, kappa * out[start + HALF : start + SLAB]], 0))
    return slabs


def all_faces(field, kappa, pair_trace_ref, trace_ref):
    high, low = parts_of(field, 2)
    triple = jnp.concatenate([high, low, high], 0)
    out = dot(trace_ref[...], triple)
    slabs = face_rows(dot(pair_trace_ref[...], triple), kappa, 2) + face_rows(out, kappa, FACES - 2)
    return slabs, kappa * out[(FACES - 2) * SLAB :]


def moved_ghosts(records, lists, trace_ref):
    columns = records.T
    slabs = face_rows(times3(trace_ref[...], columns), columns[BLOCK : BLOCK + 1], 2)
    slots = records[:, BLOCK + 1 : BLOCK + 2]
    side_of = lax.broadcasted_iota(jnp.int32, (2 * MOVE, 1), 0) // MOVE
    found = []
    for side in range(2):
        wanted = jnp.where(side_of == side, slots, -1.0)
        found.append(pick(slabs[1 - side], as_bf16(jnp.where(wanted == lists[side], 1.0, 0.0)), 2))
    return found


def face_jumps(face, near, own, kappa, neighbour_ref, code_ref, flips):
    code = code_ref[face : face + 1]
    first = 1.0 - 2.0 * as_f32(jnp.bitwise_and(code, 1))
    second = 1.0 - 2.0 * as_f32(jnp.right_shift(code, 1))
    sign = jnp.where(flips[:HALF, 0:1] > 0.0, first, 1.0) * jnp.where(flips[:HALF, 1:2] > 0.0, second, 1.0)
    outside = jnp.where(neighbour_ref[face : face + 1] < 0, 2.0, 1.0)
    strength = PENALTY * jnp.maximum(kappa, near[FACE : FACE + 1])
    values = outside * own[:HALF] - sign * near[:HALF]
    return values, outside * own[HALF:] - sign * near[HALF:], strength


def face_terms(jumps, kappa):
    values, fluxes, strength = jumps
    return jnp.concatenate([strength * values - 0.5 * fluxes, kappa * values], 0)


def one_sided(jumps, own):
    values, fluxes, strength = jumps
    return own[:HALF] * (strength * values - 0.5 * fluxes) - 0.5 * own[HALF:] * values


def both_sided(jumps):
    values, fluxes, strength = jumps
    return values * (strength * values - fluxes)


def first_kernel(placed_ref, slab_ref, beside_ref, stiff_ref, near_up_ref, near_down_ref, far_up_ref, far_down_ref, packed_ref, pair_trace_ref,
                 neighbour_ref, code_ref, trace_ref, back_ref, back_ghost_ref, weight_ref, flip_ref, send_hot_ref,
                 ghost_hot_ref, field_ref, kappa_ref, image_ref, pair_ref, right_ref):
    cells = placed_ref.shape[1]
    buffers = (near_up_ref[...], near_down_ref[...])
    records = jnp.concatenate(
        [piece for buffer in buffers for piece in (buffer[THIN:, :LANES], buffer[THIN:, LANES:])], 0
    )
    slot = records[:, BLOCK + 1 : BLOCK + 2].astype(jnp.int32) - 1
    slot = jnp.where(slot < 0, -2, slot)
    ids = lax.broadcasted_iota(jnp.int32, (2 * MOVE, cells), 1)
    arrived = records.T
    new_slabs, new_stiff = all_faces(arrived, arrived[BLOCK : BLOCK + 1], pair_trace_ref, trace_ref)
    added = pick(jnp.concatenate([*new_slabs, new_stiff, arrived], 0), as_bf16(jnp.where(ids == slot, 1.0, 0.0)), 2)
    merged = placed_ref[...] + added[FACES * SLAB + ROWS :]
    kappa = merged[BLOCK : BLOCK + 1]
    row = lax.broadcasted_iota(jnp.int32, (ROWS, 1), 0)
    field = jnp.where(row < BLOCK, merged, 0.0)
    field_ref[...] = field
    kappa_ref[...] = kappa
    slabs = [
        slab_ref[face * SLAB : (face + 1) * SLAB] + added[face * SLAB : (face + 1) * SLAB] for face in range(FACES)
    ]
    stiff = stiff_ref[...] + added[FACES * SLAB : FACES * SLAB + ROWS]
    lists = [buffer[LIST : LIST + 1] for buffer in buffers]
    far = jnp.concatenate([far_up_ref[...], far_down_ref[...]], 0)
    moved = [moved_ghosts(some, lists, pair_trace_ref) for some in (packed_ref[...], far)]
    flips = flip_ref[...]
    terms = []
    for face in range(FACES):
        chosen = as_bf16(jnp.where(slot == neighbour_ref[face : face + 1], 1.0, 0.0))
        near = beside_ref[face * SLAB : (face + 1) * SLAB] + pick(new_slabs[face ^ 1], chosen, 2)
        if face < 2:
            ghosts = spread(buffers[face][:THIN]) + (moved[0][face] + moved[1][face])
            near = near + pick(ghosts, ghost_hot_ref[face], 2)
        jumps = face_jumps(face, near, slabs[face], kappa, neighbour_ref, code_ref, flips)
        terms.append(face_terms(jumps, kappa))
    volume = weight_ref[...] * field + stiff
    image = (volume + times3(back_ref[...], jnp.concatenate(terms[2:], 0))
             + times3(back_ghost_ref[...], jnp.concatenate(terms[:2], 0)))
    image_ref[...] = image
    pair_ref[:SLAB], pair_ref[SLAB:] = face_rows(times3(pair_trace_ref[...], image), kappa, 2)
    right_ref[...] = squeeze(pick(pair_ref[SLAB:], send_hot_ref[1], 2))


def whole_sum(value):
    return jnp.sum(jnp.sum(value, axis=0, keepdims=True), axis=1, keepdims=True)


def second_kernel(image_ref, kappa_ref, pair_ref, neighbour_ref, code_ref, trace_ref, back_ref, weight_ref,
                  flip_ref, hot_ref, send_hot_ref, field_ref, part_ref, near_ref, sums_ref, left_ref):
    left_ref[...] = squeeze(pick(pair_ref[:SLAB], send_hot_ref[0], 2))
    cells = image_ref.shape[1]
    kappa = kappa_ref[...]
    flips = flip_ref[...]
    field, image = field_ref[...], image_ref[...]
    out = times3(trace_ref[...], image)
    slabs = face_rows(out, kappa, FACES - 2)
    total = jnp.zeros((HALF, cells), jnp.float32)
    terms = []
    for face in range(FACES):
        slab = pair_ref[(1 - face) * SLAB : (2 - face) * SLAB] if face < 2 else slabs[(face ^ 1) - 2]
        near = pick(slab, hot_ref[face], 2)
        if face < 2:
            near_ref[face * SLAB : (face + 1) * SLAB] = near
        if face == 0:
            continue
        own = pair_ref[SLAB:] if face == 1 else slabs[face - 2]
        jumps = face_jumps(face, near, own, kappa, neighbour_ref, code_ref, flips)
        share = one_sided(jumps, own)
        if face == 1:
            total = total + jnp.where(neighbour_ref[1:2] < cells, share, 0.0)
        else:
            total = total + share
            terms.append(face_terms(jumps, kappa))
    volume = weight_ref[...] * image + kappa * out[(FACES - 2) * SLAB :]
    part_ref[...] = volume + times3(back_ref[...], jnp.concatenate(terms, 0))
    totals = (whole_sum(field * field), whole_sum(field * image), whole_sum(image * image),
              whole_sum(image * volume) + whole_sum(flips[:HALF, 2:3] * total))
    lane = lax.broadcasted_iota(jnp.int32, (1, LANES), 1)
    sums = jnp.zeros((1, LANES), jnp.float32)
    for place, value in enumerate(totals):
        sums = jnp.where(lane == place, value, sums)
    sums_ref[...] = sums


def squeeze(slab):
    idle = jnp.zeros((THIN - 2 * FACE - 1, slab.shape[1]), jnp.float32)
    return jnp.concatenate([slab[: FACE + 1], slab[HALF : HALF + FACE], idle], 0)


def spread(thin):
    gap = jnp.zeros((HALF - FACE - 1, thin.shape[1]), jnp.float32)
    tail = jnp.zeros((HALF - FACE, thin.shape[1]), jnp.float32)
    return jnp.concatenate([thin[: FACE + 1], gap, thin[FACE + 1 : 2 * FACE + 1], tail], 0)


def ghost_jumps(face, ghosts, near_ref, pair_ref, kappa, neighbour_ref, code_ref, flips, ghost_hot_ref):
    rows = slice(face * SLAB, (face + 1) * SLAB)
    near = near_ref[rows] + pick(ghosts, ghost_hot_ref[face], 2)
    return face_jumps(face, near, pair_ref[rows], kappa, neighbour_ref, code_ref, flips)


def energy_kernel(near_ref, pair_ref, kappa_ref, from_left_ref, neighbour_ref, code_ref, flip_ref,
                  ghost_hot_ref, partial_ref, sums_ref, term_ref):
    cells = near_ref.shape[1]
    kappa = kappa_ref[...]
    flips = flip_ref[...]
    jumps = ghost_jumps(0, spread(from_left_ref[...]), near_ref, pair_ref, kappa, neighbour_ref, code_ref, flips,
                        ghost_hot_ref)
    term_ref[...] = face_terms(jumps, kappa)
    shared = jnp.where(neighbour_ref[0:1] < cells, one_sided(jumps, pair_ref[:SLAB]), both_sided(jumps))
    total = whole_sum(flips[:HALF, 2:3] * shared)
    lane = lax.broadcasted_iota(jnp.int32, (1, LANES), 1)
    sums = partial_ref[...] + jnp.where(lane == 3, total, 0.0)
    sums_ref[...] = jnp.broadcast_to(sums, sums_ref.shape)


def update_kernel(sums_ref, field_ref, image_ref, part_ref, edge_ref, near_ref, pair_ref, kappa_ref,
                  from_right_ref, neighbour_ref, code_ref, back_ref, flip_ref, ghost_hot_ref,
                  solution_hbm, residual_hbm, solution, residual, sems):
    sums = sums_ref[...]
    bb, bw, ww, wt = (sums[:, place : place + 1] for place in range(4))
    alpha = bb / bw
    rr = bb - 2.0 * alpha * bw + alpha * alpha * ww
    beta = rr / bb
    more = 1.0 + beta
    inner = more * more * bw - 2.0 * alpha * more * ww + alpha * alpha * wt
    step = rr / inner
    field, image = field_ref[:BLOCK], image_ref[:BLOCK]
    solution[...] = (alpha + step * more) * field - (step * alpha) * image
    first = pltpu.make_async_copy(solution, solution_hbm, sems.at[0])
    first.start()
    kappa = kappa_ref[...]
    jumps = ghost_jumps(1, spread(from_right_ref[...]), near_ref, pair_ref, kappa, neighbour_ref, code_ref,
                        flip_ref[...], ghost_hot_ref)
    edges = jnp.concatenate([edge_ref[...], face_terms(jumps, kappa)], 0)
    twice = part_ref[...] + times3(back_ref[...], edges)
    residual[...] = field - (alpha + step * more) * image + (step * alpha) * twice[:BLOCK]
    second = pltpu.make_async_copy(residual, residual_hbm, sems.at[1])
    second.start()
    first.wait()
    second.wait()


def shift(value, distance):
    count = lax.axis_size(AXES)
    return lax.ppermute(value, AXES, [(i, (i + distance) % count) for i in range(count)])


def bf16(*shape):
    return jax.ShapeDtypeStruct(shape, jnp.bfloat16)


def i32(*shape):
    return jax.ShapeDtypeStruct(shape, jnp.int32)


def body(right_side, conductivity, destination, neighbour, orientation, send_list):
    constants = (jnp.asarray(table) for table in operator_constants())
    trace_pair, trace_rest, back_ghost, back_local, weight_rows, flips = constants
    devices = lax.axis_size(AXES)
    cells = destination.shape[0]
    ghosts = send_list.shape[1]
    whole, slab, row = f32(ROWS, cells), f32(THIN, ghosts), f32(1, cells)
    pair = f32(2 * SLAB, cells)
    big = 2 * ROWS * cells
    near_up, near_down, far_up, far_down, packed, payload, stay, send, nbr, trace_pair = call(
        pack_kernel,
        [f32(THIN + MOVE // 2, ghosts)] * 2 + [f32(MOVE, ROWS)] * 2
        + [f32(2 * MOVE, ROWS), whole, i32(1, cells), i32(2, ghosts), i32(FACES, cells), bf16(*trace_pair.shape)],
        [right_side, conductivity[None], destination[None], send_list, trace_pair, neighbour], big * LANES * 6,
        [pltpu.VMEM((BLOCK, cells), jnp.float32), pltpu.VMEM((1, cells), jnp.float32),
         pltpu.VMEM((1, cells), jnp.int32), pltpu.SemaphoreType.DMA((6,))],
        far=6)
    near_up = shift(near_up, 1)
    far_up = shift(far_up, 2)
    far_down = shift(far_down, -2)
    near_down = shift(near_down, -1)
    later = [orientation, trace_rest, back_local, back_ghost, weight_rows, flips]
    slabs = f32(FACES * SLAB, cells)
    placed, send_hot, ghost_hot, hot, slab_rows, beside, stiff, *later = call(
        functools.partial(stay_kernel, len(later)),
        [whole, bf16(2, cells, ghosts), bf16(2, ghosts, cells), bf16(FACES, cells, cells), slabs, slabs, whole]
        + [jax.ShapeDtypeStruct(a.shape, a.dtype) for a in later],
        later + [payload, stay, send, nbr, trace_pair], big * cells * 3, [pltpu.SemaphoreType.DMA((len(later),))],
        far=len(later))
    orientation, trace_rest, back_local, back_ghost, weight_rows, flips = later
    field, kappa, image, faces, right = call(
        first_kernel, [whole, row, whole, pair, slab],
        [placed, slab_rows, beside, stiff, near_up, near_down, far_up, far_down, packed, trace_pair, nbr, orientation, trace_rest,
         back_local, back_ghost, weight_rows, flips, send_hot, ghost_hot],
        big * cells * FACES * 2, ())
    from_left = shift(right, 1)
    part, near, partial, left = call(
        second_kernel, [whole, pair, f32(1, LANES), slab],
        [image, kappa, faces, nbr, orientation, trace_rest, back_local, weight_rows, flips, hot, send_hot, field],
        big * cells * FACES * 2, ())
    from_right = shift(left, -1)
    sums, edge = call(
        energy_kernel, [f32(devices, LANES), f32(SLAB, cells)],
        [near, faces, kappa, from_left, nbr, orientation, flips, ghost_hot, partial],
        big * SLAB * 2, ())
    sums = lax.all_to_all(sums, AXES, 0, 0, tiled=True)
    total = jnp.sum(sums, axis=0, keepdims=True)
    return tuple(call(
        update_kernel, [f32(BLOCK, cells)] * 2,
        [total, field, image, part, edge, near, faces, kappa, from_right, nbr, orientation, back_ghost, flips,
         ghost_hot], big * 2 * SLAB * 3,
        [pltpu.VMEM((BLOCK, cells), jnp.float32)] * 2 + [pltpu.SemaphoreType.DMA((2,))], out=pltpu.MemorySpace.HBM))


def solution(mesh):
    in_specs = (
        P(None, AXES),
        P(AXES),
        P(AXES),
        P(None, AXES),
        P(None, AXES),
        P(None, AXES),
    )
    out_specs = (P(None, AXES), P(None, AXES))
    return jax.shard_map(body, mesh=mesh, in_specs=in_specs, out_specs=out_specs, check_vma=False)
```
